32 devices in a mesh: batch: 4 (over y, x), ctx: 8 (over z, core).
Axes of the slice: x: 2, y: 2, z: 4, core: 2. Of those that a mesh axis runs over, the one named last changes fastest.
Arguments:
- asked_for: bfloat16 [4, 1024, 64, 64], P('batch', 'ctx'), may hold values from -6 to 6
- offered: bfloat16 [4, 1024, 64, 64], P('batch', 'ctx'), may hold values from -6 to 6
- contents: bfloat16 [4, 1024, 64, 64], P('batch', 'ctx'), may hold values from -6 to 6
- out_weight: bfloat16 [4096, 4096], P('batch'), may hold values from -0.09375 to 0.09375
Outputs:
- layer_out: bfloat16 [4, 1024, 4096], P('batch', 'ctx')
The draws below stay inside these ranges and needn't reach their ends.
All inputs are finite; a program needn't handle non-finite values.
Results may differ from the reference program's by a relative error of at most 0.006.
Values may be sent and summed in bfloat16 or wider, within the bound.
A program may use at most 128 MiB of HBM per device.

```python
import jax
import jax.numpy as jnp
from jax import lax

HEADS = 64
HEAD_SIZE = 64
BATCH = 4
TOKENS = 1024
WIDTH = 4096


def shard_levels(key, dims, split, least, top_value):
    level = 1.0
    for axis_at, shards_of in split:
        steps = jax.random.uniform(jax.random.fold_in(jax.random.fold_in(key, 6), axis_at), (shards_of,), jnp.float32, least / len(split), top_value / len(split))
        level = level * jnp.repeat(jnp.exp(steps), dims[axis_at] // shards_of).reshape((-1,) + (1,) * (len(dims) - 1 - axis_at))
    return level


def centred(rng, extent, width, bound, pieces=(), kind=jnp.bfloat16):
    entries = jax.random.normal(rng, extent, jnp.float32) * width
    if len(pieces) > 0:
        entries = shard_levels(rng, extent, pieces, -0.22, 0.18) * entries
    return jnp.clip(entries, min=-bound, max=bound).astype(kind)


def setup_inputs(seed: int = 0) -> dict:
    key_of = jax.random.split(jax.random.key(seed), 5)
    return {
        "asked_for": centred(key_of[0], (BATCH, TOKENS, HEADS, HEAD_SIZE), 1.0, 6.0, ((0, 4), (1, 8))),
        "offered": centred(key_of[1], (BATCH, TOKENS, HEADS, HEAD_SIZE), 1.0, 6.0, ((0, 4), (1, 8))),
        "contents": centred(key_of[2], (BATCH, TOKENS, HEADS, HEAD_SIZE), 1.0, 6.0, ((0, 4), (1, 8))),
        "out_weight": centred(key_of[3], (WIDTH, WIDTH), WIDTH ** -0.5, 0.09375, ((0, 4),)),
    }


def to_features(values):
    wide = values.astype(jnp.float32)
    return (jax.nn.softplus(wide)).astype(jnp.bfloat16)


def after_reading(read, count):
    result = read * count ** 0.5
    return result.astype(jnp.bfloat16)


def look_up(features, state, mass):
    small = lax.optimization_barrier(state.astype(jnp.bfloat16))
    top = jnp.einsum("bthd,bhde->bthe", features.astype(jnp.float32), small.astype(jnp.float32))
    bottom = jnp.einsum("bthd,bhd->bth", features.astype(jnp.float32), mass, precision=lax.Precision.HIGHEST)
    return top / (bottom + 1e-3)[..., None]


def reference(asked_for, offered, contents, out_weight):
    query_feature, key_feature = lax.optimization_barrier((to_features(asked_for), to_features(offered)))
    state = jnp.einsum("bthd,bthe->bhde", key_feature.astype(jnp.float32), contents.astype(jnp.float32)) / TOKENS
    mass = jnp.sum(key_feature.astype(jnp.float32), axis=1) / TOKENS
    mixed = after_reading(look_up(query_feature, state, mass), TOKENS).reshape(BATCH, TOKENS, WIDTH)
    mixed = lax.optimization_barrier(mixed)
    layer_out = jnp.einsum("btw,wv->btv", mixed.astype(jnp.float32), out_weight.astype(jnp.float32)).astype(jnp.bfloat16)
    return layer_out
```

```python
import functools
import math

import jax
import jax.numpy as jnp
from jax import lax
from jax.experimental import pallas as pl
from jax.experimental.pallas import tpu as pltpu
from jax.sharding import PartitionSpec as P

MESH = pl.DeviceIdType.MESH
LANES = 128
EXTRA = 8
CHUNK = 512


def softplus(x):
    x = x.astype(jnp.float32)
    return (jnp.maximum(x, 0.0) + jnp.log(1.0 + jnp.exp(-jnp.abs(x)))).astype(jnp.bfloat16)


def kernel(
    ny, nx, nc, size, grid, q_ref, k_ref, v_ref, w_ref, o_ref,
    kt, vt, wv, qx, ft, part, part_in, both, rs, own, st, mixed, mine, stage1, stage2,
    local_sem, q_send, q_recv, pa_send, pa_recv, rs_send, rs_recv,
    ag_send, ag_recv, fw_send, fw_recv,
):
    b, c = lax.axis_index("batch"), lax.axis_index("ctx")
    nb = ny * nx
    rows, tokens = k_ref.shape
    pairs = rows // LANES
    ppg = pairs // nb
    group = rows // nb
    messages, held, spread = grid
    blocks = ppg // held
    base = held * size
    total = nb * nc
    me = b * nc + c
    count = tokens * nc
    chunks = mine[0].shape[0]
    nz, z_me, odd = nc // 2, c // 2, lax.rem(c, 2)
    partner = z_me * 2 + 1 - odd
    y_me, x_me = b // nx, lax.rem(b, nx)

    k_copy = pltpu.make_async_copy(k_ref, kt, local_sem.at[0])
    v_copy = pltpu.make_async_copy(v_ref, vt, local_sem.at[1])
    q_copy = pltpu.make_async_copy(q_ref.at[pl.ds(b * group, group)], qx.at[0], local_sem.at[2])
    w_copy = pltpu.make_async_copy(w_ref, wv, local_sem.at[3])
    k_copy.start()
    v_copy.start()
    q_copy.start()
    w_copy.start()

    barrier = pltpu.get_barrier_semaphore()

    def greet(i, carry):
        d = lax.rem(me + i, total)
        pl.semaphore_signal(barrier, inc=1, device_id=(d // nc, lax.rem(d, nc)), device_id_type=MESH)
        return carry

    lax.fori_loop(1, total, greet, 0)

    def ahead(k):
        return lax.rem(y_me + k // nx, ny) * nx + lax.rem(x_me + k % nx, nx)

    def back(k):
        return (ny - k // nx) % ny * nx + (nx - k % nx) % nx

    def q_move(k):
        to = ahead(k)
        return pltpu.make_async_remote_copy(
            src_ref=q_ref.at[pl.ds(to * group, group)], dst_ref=qx.at[back(k)],
            send_sem=q_send.at[k], recv_sem=q_recv.at[back(k)],
            device_id=(to, c), device_id_type=MESH,
        )

    lane = lax.broadcasted_iota(jnp.int32, (size, LANES), 1) < size
    row_x = lax.broadcasted_iota(jnp.int32, (EXTRA, LANES), 0)
    ones = jnp.ones((2 * EXTRA, tokens), jnp.bfloat16)

    def first_pair(j, owner):
        if spread:
            return (lax.rem(owner, 2) * messages + j) * ppg + owner // 2 * held
        return j * nc + owner

    def pa_move(j, k):
        return pltpu.make_async_remote_copy(
            src_ref=part.at[j, k - 1], dst_ref=part_in.at[j, k - 1],
            send_sem=pa_send.at[j, k - 1], recv_sem=pa_recv.at[j, k - 1],
            device_id=(b, partner), device_id_type=MESH,
        )

    def rs_move(j, k):
        return pltpu.make_async_remote_copy(
            src_ref=both.at[j, k - 1], dst_ref=rs.at[j, k - 1],
            send_sem=rs_send.at[j, k - 1], recv_sem=rs_recv.at[j, k - 1],
            device_id=(b, lax.rem(z_me + k, nz) * 2 + odd), device_id_type=MESH,
        )

    def partial_sum(p):
        at = pl.multiple_of(p * LANES, LANES)
        feature = softplus(kt[pl.ds(at, LANES), :])
        left = jnp.concatenate([vt[pl.ds(at, LANES), :], ones], axis=0)
        s = lax.dot_general(left, feature, (((1,), (1,)), ((), ())), preferred_element_type=jnp.float32)
        return jnp.where(lane, s[:size], s[size : 2 * size]), s[2 * size : 2 * size + EXTRA]

    def split_mass(masses):
        packed = jnp.zeros((EXTRA, LANES), jnp.float32)
        for t, m in enumerate(masses):
            high = m.astype(jnp.bfloat16).astype(jnp.float32)
            packed = jnp.where(row_x == 2 * t, high, jnp.where(row_x == 2 * t + 1, m - high, packed))
        return packed.astype(jnp.bfloat16)

    def states_of(block):
        return [block[t * size : (t + 1) * size].astype(jnp.float32) for t in range(held)]

    def masses_of(block):
        extra = block[base:].astype(jnp.float32)
        return [extra[2 * t : 2 * t + 1] + extra[2 * t + 1 : 2 * t + 2] for t in range(held)]

    k_copy.wait()
    v_copy.wait()

    for j in range(messages):

        def for_partner(k, carry):
            owner = lax.rem(z_me + k, nz) * 2 + 1 - odd
            sums = [partial_sum(first_pair(j, owner) + t) for t in range(held)]
            for t, (state, _) in enumerate(sums):
                part[j, k - 1, t * size : (t + 1) * size, :] = state.astype(jnp.bfloat16)
            part[j, k - 1, base:, :] = split_mass([m for _, m in sums])
            return carry

        lax.fori_loop(1, nz + 1, for_partner, 0)

    pl.semaphore_wait(barrier, total - 1)

    for j in range(messages):
        for k in range(1, nz + 1):
            pa_move(j, k).start()
    for k in range(1, nb):
        q_move(k).start()

    for j in range(messages):

        def for_chip(k, carry):
            owner = lax.rem(z_me + k, nz) * 2 + odd
            sums = [partial_sum(first_pair(j, owner) + t) for t in range(held)]
            pa_move(j, k).wait_recv()
            block = part_in[j, k - 1]
            for t, ((state, _), other) in enumerate(zip(sums, states_of(block))):
                both[j, k - 1, t * size : (t + 1) * size, :] = (state + other).astype(jnp.bfloat16)
            both[j, k - 1, base:, :] = split_mass([m + o for (_, m), o in zip(sums, masses_of(block))])

            @pl.when(k < nz)
            def _():
                rs_move(j, k).start()

            return carry

        lax.fori_loop(1, nz + 1, for_chip, 0)

    def features(k):
        def featured(i, carry):
            at = pl.multiple_of(i * LANES, LANES)
            ft[k, i] = softplus(qx[k, pl.ds(at, LANES), :]).T
            return carry

        lax.fori_loop(0, ppg, featured, 0)

    q_copy.wait()
    features(0)

    def ag_move(j, k):
        p = first_pair(j, c)
        g = p // ppg
        block = lax.rem(p, ppg) // held
        side = lax.rem(block, 2)
        to = lax.rem(z_me + k, nz) * 2 + side
        landing = b * blocks + block
        remote = pltpu.make_async_remote_copy(
            src_ref=own.at[j], dst_ref=st.at[landing],
            send_sem=ag_send.at[j * nz + k], recv_sem=ag_recv.at[landing],
            device_id=(g, to), device_id_type=MESH,
        )
        local = pltpu.make_async_copy(own.at[j], st.at[landing], ag_recv.at[landing])
        here = jnp.logical_and(g == b, side == odd)
        return here, remote, local

    for j in range(messages):
        for k in range(1, nz):
            rs_move(j, k).wait_recv()
        parts = [both[j, nz - 1]] + [rs[j, k - 1] for k in range(1, nz)]
        states = [sum(x) / count for x in zip(*[states_of(p) for p in parts])]
        masses = [sum(x) / count for x in zip(*[masses_of(p) for p in parts])]
        for t, state in enumerate(states):
            own[j, t * size : (t + 1) * size, :] = state.astype(jnp.bfloat16)
        own[j, base:, :] = split_mass([jnp.broadcast_to(m, (EXTRA, LANES)) for m in masses])
        for k in range(1, nz):
            ag_move(j, k)[1].start()
        here, remote, local = ag_move(j, 0)
        pl.when(jnp.logical_not(here))(remote.start)
        pl.when(here)(local.start)

    for k in range(1, nb):
        q_move(back(k)).wait_recv()
        features(k)

    def fw_move(k, u):
        landing = ahead(k) * blocks + 2 * u + odd
        return pltpu.make_async_remote_copy(
            src_ref=st.at[landing], dst_ref=st.at[landing],
            send_sem=fw_send.at[landing], recv_sem=fw_recv.at[landing],
            device_id=(b, partner), device_id_type=MESH,
        )

    def read(k, block):
        at = ahead(k) * blocks + block
        for t in range(held):
            state = st[at, t * size : (t + 1) * size, :]
            mass = st[at, base:, :].astype(jnp.float32)
            mass = jnp.broadcast_to(mass[2 * t : 2 * t + 1], (size, LANES)).astype(jnp.bfloat16)
            zero = jnp.zeros_like(state)
            right = jnp.concatenate(
                [jnp.where(lane, x, zero) if low else jnp.where(lane, zero, x)
                 for x in (state, mass) for low in (True, False)], axis=0,
            )
            slot = block * held + t
            y = lax.dot_general(
                ft[k, slot], right, (((1,), (1,)), ((), ())), preferred_element_type=jnp.float32
            )
            y = y[:, :LANES] * (count**0.5 / (y[:, LANES:] + 0.001))
            column = pl.multiple_of(slot * LANES, LANES)
            mixed[k * tokens : (k + 1) * tokens, pl.ds(column, LANES)] = y.astype(jnp.bfloat16)

    for u in range(blocks // 2):
        for k in range(nb):
            at = ahead(k) * blocks + 2 * u + odd
            pltpu.make_async_copy(st.at[at], st.at[at], ag_recv.at[at]).wait()
            fw_move(k, u).start()
            read(k, 2 * u + odd)
    for u in range(blocks // 2):
        for k in range(nb):
            at = ahead(k) * blocks + 2 * u + 1 - odd
            pltpu.make_async_copy(st.at[at], st.at[at], fw_recv.at[at]).wait()
            read(k, 2 * u + 1 - odd)

    w_copy.wait()

    width = o_ref.shape[1] // chunks
    half = width // 2

    def place(axis, k):
        if axis == 0:
            return (y_me * nx + lax.rem(x_me + k, nx), c)
        return (lax.rem(y_me + k, ny) * nx + x_me, c)

    def offset(axis, k, other):
        return (other * nx + k) if axis == 0 else (k * nx + other)

    def first_move(j, h, k):
        n2 = ny if h == 0 else nx
        at = pl.ds((k - 1) * n2, n2)
        out_buf, in_buf, send, recv = stage1[h]
        return pltpu.make_async_remote_copy(
            src_ref=out_buf.at[j, at], dst_ref=in_buf.at[j, at],
            send_sem=send.at[j, k - 1], recv_sem=recv.at[j, k - 1],
            device_id=place(h, k), device_id_type=MESH,
        )

    def second_move(j, h, k):
        out_buf, in_buf, send, recv = stage2[h]
        return pltpu.make_async_remote_copy(
            src_ref=out_buf.at[j, k - 1], dst_ref=in_buf.at[j, k - 1],
            send_sem=send.at[j, k - 1], recv_sem=recv.at[j, k - 1],
            device_id=place(1 - h, k), device_id_type=MESH,
        )

    sizes = ((nx, ny), (ny, nx))

    def project(j, carry):
        at = pl.multiple_of(j * width, width)
        y = jnp.dot(mixed[...], wv[:, pl.ds(at, width)], preferred_element_type=jnp.float32)
        for h, (n1, n2) in enumerate(sizes):
            for k in range(n1):
                for other in range(n2):
                    r = offset(h, k, other) * tokens
                    piece = y[r : r + tokens, h * half : (h + 1) * half]
                    if k > 0:
                        stage1[h][0][j, (k - 1) * n2 + other] = piece.astype(jnp.bfloat16)
                    else:
                        mine[h][j, other] = piece
        for h, (n1, n2) in enumerate(sizes):
            for k in range(1, n1):
                first_move(j, h, k).start()
        return carry

    lax.fori_loop(0, chunks, project, 0)

    def relay(j, carry):
        for h, (n1, n2) in enumerate(sizes):
            for k in range(1, n1):
                first_move(j, h, k).wait_recv()
            for other in range(n2):
                y = mine[h][j, other]
                for k in range(1, n1):
                    y = y + stage1[h][1][j, (k - 1) * n2 + other].astype(jnp.float32)
                if other > 0:
                    stage2[h][0][j, other - 1] = y.astype(jnp.bfloat16)
                else:
                    mine[h][j, 0] = y
        for h, (n1, n2) in enumerate(sizes):
            for k in range(1, n2):
                second_move(j, h, k).start()
        return carry

    lax.fori_loop(0, chunks, relay, 0)

    def collect(j, carry):
        for h, (n1, n2) in enumerate(sizes):
            at = pl.multiple_of(j * width + h * half, half)
            y = mine[h][j, 0]
            for k in range(1, n2):
                second_move(j, h, k).wait_recv()
                y = y + stage2[h][1][j, k - 1].astype(jnp.float32)
            o_ref[:, pl.ds(at, half)] = y.astype(jnp.bfloat16)
        return carry

    lax.fori_loop(0, chunks, collect, 0)

    for k in range(1, nb):
        q_move(k).wait_send()

    for j in range(messages):
        for k in range(1, nz + 1):
            pa_move(j, k).wait_send()
        for k in range(1, nz):
            rs_move(j, k).wait_send()
            ag_move(j, k)[1].wait_send()
        here, remote, _ = ag_move(j, 0)
        pl.when(jnp.logical_not(here))(remote.wait_send)
    for k in range(nb):
        for u in range(blocks // 2):
            fw_move(k, u).wait_send()

    def pr_end(j, carry):
        for h, (n1, n2) in enumerate(sizes):
            for k in range(1, n1):
                first_move(j, h, k).wait_send()
            for k in range(1, n2):
                second_move(j, h, k).wait_send()
        return carry

    lax.fori_loop(0, chunks, pr_end, 0)


def solution(mesh):
    nb, nc = mesh.shape["batch"], mesh.shape["ctx"]
    nx = next(n for n in range(math.isqrt(nb), 0, -1) if nb % n == 0)
    ny = nb // nx

    def shards(asked_for, offered, contents, out_weight):
        _, tokens, heads, size = asked_for.shape
        rows = heads * size
        depth, columns = out_weight.shape
        pairs = rows // LANES
        width = CHUNK if columns % CHUNK == 0 else columns
        chunks = columns // width

        def flat(x):
            return x.transpose(0, 2, 3, 1).reshape(rows, tokens)

        bf16, f32 = jnp.bfloat16, jnp.float32
        dma = pltpu.SemaphoreType.DMA
        sizes = ((nx, ny), (ny, nx))

        def stage(blocks, moves):
            buffer = pltpu.VMEM((chunks, blocks, tokens, width // 2), bf16)
            return [buffer, buffer, dma((chunks, moves)), dma((chunks, moves))]

        half_pairs, ppg = nc // 2, pairs // nb
        spread = nb % 2 == 0 and ppg % half_pairs == 0 and ppg >= half_pairs
        held = ppg // half_pairs if spread else 1
        messages = pairs // nc // held
        high = held * size + EXTRA
        hops = pltpu.VMEM((messages, nc // 2, high, LANES), bf16)
        scratch = [
            pltpu.VMEM((rows, tokens), bf16),
            pltpu.VMEM((rows, tokens), bf16),
            pltpu.VMEM((depth, columns), bf16),
            pltpu.VMEM((nb, rows // nb, tokens), bf16),
            pltpu.VMEM((nb, ppg, tokens, LANES), bf16),
            hops,
            hops,
            hops,
            hops,
            pltpu.VMEM((messages, high, LANES), bf16),
            pltpu.VMEM((pairs // held, high, LANES), bf16),
            pltpu.VMEM((nb * tokens, rows // nb), bf16),
            [pltpu.VMEM((chunks, n2, tokens, width // 2), f32) for _, n2 in sizes],
            [stage((n1 - 1) * n2, n1 - 1) for n1, n2 in sizes],
            [stage(n2 - 1, n2 - 1) for _, n2 in sizes],
            dma((4,)),
            dma((nb,)),
            dma((nb,)),
            dma((messages, nc // 2)),
            dma((messages, nc // 2)),
            dma((messages, nc // 2)),
            dma((messages, nc // 2)),
            dma((messages * nc // 2,)),
            dma((pairs // held,)),
            dma((pairs // held,)),
            dma((pairs // held,)),
        ]
        buffers = [x for x in jax.tree.leaves(scratch, is_leaf=lambda x: hasattr(x, "shape")) if x.dtype in (bf16, f32)]
        used = sum(math.prod(x.shape) * jnp.dtype(x.dtype).itemsize for x in buffers)
        limit = used + 4 * tokens * columns + 3 * 2**20

        out = pl.pallas_call(
            functools.partial(kernel, ny, nx, nc, size, (messages, held, spread)),
            out_shape=jax.ShapeDtypeStruct((tokens, columns), bf16),
            in_specs=[pl.BlockSpec(memory_space=pl.ANY)] * 4,
            out_specs=pl.BlockSpec(memory_space=pltpu.VMEM),
            scratch_shapes=scratch,
            compiler_params=pltpu.CompilerParams(
                collective_id=0, has_side_effects=True, vmem_limit_bytes=max(limit, 52 * 2**20)
            ),
        )(flat(asked_for), flat(offered), flat(contents), out_weight)
        return out[None]

    in_specs = (
        P("batch", "ctx", None, None),
        P("batch", "ctx", None, None),
        P("batch", "ctx", None, None),
        P("batch", None),
    )
    return jax.shard_map(
        shards, mesh=mesh, in_specs=in_specs, out_specs=P("batch", "ctx", None), check_vma=False
    )
```

```python
import functools
import math

import jax
import jax.numpy as jnp
from jax import lax
from jax.experimental import pallas as pl
from jax.experimental.pallas import tpu as pltpu
from jax.sharding import PartitionSpec as P

MESH = pl.DeviceIdType.MESH
LANES = 128
EXTRA = 8
CHUNK = 512


def softplus(x):
    x = x.astype(jnp.float32)
    return (jnp.maximum(x, 0.0) + jnp.log(1.0 + jnp.exp(-jnp.abs(x)))).astype(jnp.bfloat16)


def kernel(
    ny, nx, nc, size, grid, q_ref, k_ref, v_ref, w_ref, o_ref,
    kt, vt, wv, qx, ft, part, part_in, both, rs, own, st, mixed, mine, stage1, stage2,
    local_sem, q_send, q_recv, pa_send, pa_recv, rs_send, rs_recv,
    ag_send, ag_recv, fw_send, fw_recv,
):
    b, c = lax.axis_index("batch"), lax.axis_index("ctx")
    nb = ny * nx
    rows, tokens = k_ref.shape
    pairs = rows // LANES
    ppg = pairs // nb
    group = rows // nb
    messages, held, spread = grid
    blocks = ppg // held
    base = held * size
    total = nb * nc
    me = b * nc + c
    count = tokens * nc
    chunks = mine[0].shape[0]
    nz, z_me, odd = nc // 2, c // 2, lax.rem(c, 2)
    partner = z_me * 2 + 1 - odd
    y_me, x_me = b // nx, lax.rem(b, nx)

    k_copy = pltpu.make_async_copy(k_ref, kt, local_sem.at[0])
    v_copy = pltpu.make_async_copy(v_ref, vt, local_sem.at[1])
    q_copy = pltpu.make_async_copy(q_ref.at[pl.ds(b * group, group)], qx.at[0], local_sem.at[2])
    w_copy = pltpu.make_async_copy(w_ref, wv, local_sem.at[3])
    k_copy.start()
    v_copy.start()
    q_copy.start()
    w_copy.start()

    barrier = pltpu.get_barrier_semaphore()

    def greet(i, carry):
        d = lax.rem(me + i, total)
        pl.semaphore_signal(barrier, inc=1, device_id=(d // nc, lax.rem(d, nc)), device_id_type=MESH)
        return carry

    lax.fori_loop(1, total, greet, 0)

    def ahead(k):
        return lax.rem(y_me + k // nx, ny) * nx + lax.rem(x_me + k % nx, nx)

    def back(k):
        return (ny - k // nx) % ny * nx + (nx - k % nx) % nx

    near = [k for k in range(1, nb) if k < nx or k % nx == 0]
    far = [k for k in range(1, nb) if k not in near]
    order = near + far + [0]

    def q_move(k):
        to = ahead(k)
        return pltpu.make_async_remote_copy(
            src_ref=q_ref.at[pl.ds(to * group, group)], dst_ref=qx.at[back(k)],
            send_sem=q_send.at[k], recv_sem=q_recv.at[back(k)],
            device_id=(to, c), device_id_type=MESH,
        )

    lane = lax.broadcasted_iota(jnp.int32, (size, LANES), 1) < size
    row_x = lax.broadcasted_iota(jnp.int32, (EXTRA, LANES), 0)
    ones = jnp.ones((2 * EXTRA, tokens), jnp.bfloat16)

    def first_pair(j, owner):
        if spread:
            even, uneven = order[2 * j], order[2 * j + 1]
            return jnp.where(lax.rem(owner, 2) == 0, ahead(even), ahead(uneven)) * ppg + owner // 2 * held
        return j * nc + owner

    def pa_move(j, k):
        return pltpu.make_async_remote_copy(
            src_ref=part.at[j, k - 1], dst_ref=part_in.at[j, k - 1],
            send_sem=pa_send.at[j, k - 1], recv_sem=pa_recv.at[j, k - 1],
            device_id=(b, partner), device_id_type=MESH,
        )

    def rs_move(j, k):
        return pltpu.make_async_remote_copy(
            src_ref=both.at[j, k - 1], dst_ref=rs.at[j, k - 1],
            send_sem=rs_send.at[j, k - 1], recv_sem=rs_recv.at[j, k - 1],
            device_id=(b, lax.rem(z_me + k, nz) * 2 + odd), device_id_type=MESH,
        )

    def partial_sum(p):
        at = pl.multiple_of(p * LANES, LANES)
        feature = softplus(kt[pl.ds(at, LANES), :])
        left = jnp.concatenate([vt[pl.ds(at, LANES), :], ones], axis=0)
        s = lax.dot_general(left, feature, (((1,), (1,)), ((), ())), preferred_element_type=jnp.float32)
        return jnp.where(lane, s[:size], s[size : 2 * size]), s[2 * size : 2 * size + EXTRA]

    def split_mass(masses):
        packed = jnp.zeros((EXTRA, LANES), jnp.float32)
        for t, m in enumerate(masses):
            high = m.astype(jnp.bfloat16).astype(jnp.float32)
            packed = jnp.where(row_x == 2 * t, high, jnp.where(row_x == 2 * t + 1, m - high, packed))
        return packed.astype(jnp.bfloat16)

    def states_of(block):
        return [block[t * size : (t + 1) * size].astype(jnp.float32) for t in range(held)]

    def masses_of(block):
        extra = block[base:].astype(jnp.float32)
        return [extra[2 * t : 2 * t + 1] + extra[2 * t + 1 : 2 * t + 2] for t in range(held)]

    k_copy.wait()
    v_copy.wait()

    for j in range(messages):

        def for_partner(k, carry):
            owner = lax.rem(z_me + k, nz) * 2 + 1 - odd
            sums = [partial_sum(first_pair(j, owner) + t) for t in range(held)]
            for t, (state, _) in enumerate(sums):
                part[j, k - 1, t * size : (t + 1) * size, :] = state.astype(jnp.bfloat16)
            part[j, k - 1, base:, :] = split_mass([m for _, m in sums])
            return carry

        lax.fori_loop(1, nz + 1, for_partner, 0)

    pl.semaphore_wait(barrier, total - 1)

    for j in range(messages):
        for k in range(1, nz + 1):
            pa_move(j, k).start()
    for k in near:
        q_move(k).start()

    for j in range(messages):

        def for_chip(k, carry):
            owner = lax.rem(z_me + k, nz) * 2 + odd
            sums = [partial_sum(first_pair(j, owner) + t) for t in range(held)]
            pa_move(j, k).wait_recv()
            block = part_in[j, k - 1]
            for t, ((state, _), other) in enumerate(zip(sums, states_of(block))):
                both[j, k - 1, t * size : (t + 1) * size, :] = (state + other).astype(jnp.bfloat16)
            both[j, k - 1, base:, :] = split_mass([m + o for (_, m), o in zip(sums, masses_of(block))])

            @pl.when(k < nz)
            def _():
                rs_move(j, k).start()

            return carry

        lax.fori_loop(1, nz + 1, for_chip, 0)

    def features(k):
        def featured(i, carry):
            at = pl.multiple_of(i * LANES, LANES)
            ft[k, i] = softplus(qx[k, pl.ds(at, LANES), :]).T
            return carry

        lax.fori_loop(0, ppg, featured, 0)

    q_copy.wait()
    features(0)

    def ag_move(j, k):
        p = first_pair(j, c)
        g = p // ppg
        block = lax.rem(p, ppg) // held
        side = lax.rem(block, 2)
        to = lax.rem(z_me + k, nz) * 2 + side
        landing = b * blocks + block
        remote = pltpu.make_async_remote_copy(
            src_ref=own.at[j], dst_ref=st.at[landing],
            send_sem=ag_send.at[j * nz + k], recv_sem=ag_recv.at[landing],
            device_id=(g, to), device_id_type=MESH,
        )
        local = pltpu.make_async_copy(own.at[j], st.at[landing], ag_recv.at[landing])
        here = jnp.logical_and(g == b, side == odd)
        return here, remote, local

    for j in range(messages):
        for k in range(1, nz):
            rs_move(j, k).wait_recv()
        parts = [both[j, nz - 1]] + [rs[j, k - 1] for k in range(1, nz)]
        states = [sum(x) / count for x in zip(*[states_of(p) for p in parts])]
        masses = [sum(x) / count for x in zip(*[masses_of(p) for p in parts])]
        for t, state in enumerate(states):
            own[j, t * size : (t + 1) * size, :] = state.astype(jnp.bfloat16)
        own[j, base:, :] = split_mass([jnp.broadcast_to(m, (EXTRA, LANES)) for m in masses])
        for k in range(1, nz):
            ag_move(j, k)[1].start()
        here, remote, local = ag_move(j, 0)
        pl.when(jnp.logical_not(here))(remote.start)
        pl.when(here)(local.start)
        if j == 0:
            for k in far:
                q_move(k).start()
            for k in near:
                q_move(back(k)).wait_recv()
                features(k)

    def fw_move(k, u):
        landing = ahead(k) * blocks + 2 * u + odd
        return pltpu.make_async_remote_copy(
            src_ref=st.at[landing], dst_ref=st.at[landing],
            send_sem=fw_send.at[landing], recv_sem=fw_recv.at[landing],
            device_id=(b, partner), device_id_type=MESH,
        )

    def read(k, block):
        at = ahead(k) * blocks + block
        for t in range(held):
            state = st[at, t * size : (t + 1) * size, :]
            mass = st[at, base:, :].astype(jnp.float32)
            mass = jnp.broadcast_to(mass[2 * t : 2 * t + 1], (size, LANES)).astype(jnp.bfloat16)
            zero = jnp.zeros_like(state)
            right = jnp.concatenate(
                [jnp.where(lane, x, zero) if low else jnp.where(lane, zero, x)
                 for x in (state, mass) for low in (True, False)], axis=0,
            )
            slot = block * held + t
            y = lax.dot_general(
                ft[k, slot], right, (((1,), (1,)), ((), ())), preferred_element_type=jnp.float32
            )
            y = y[:, :LANES] * (count**0.5 / (y[:, LANES:] + 0.001))
            column = pl.multiple_of(slot * LANES, LANES)
            mixed[k * tokens : (k + 1) * tokens, pl.ds(column, LANES)] = y.astype(jnp.bfloat16)

    def read_all(sequences):
        for u in range(blocks // 2):
            for k in sequences:
                at = ahead(k) * blocks + 2 * u + odd
                pltpu.make_async_copy(st.at[at], st.at[at], ag_recv.at[at]).wait()
                fw_move(k, u).start()
                read(k, 2 * u + odd)
        for u in range(blocks // 2):
            for k in sequences:
                at = ahead(k) * blocks + 2 * u + 1 - odd
                pltpu.make_async_copy(st.at[at], st.at[at], fw_recv.at[at]).wait()
                read(k, 2 * u + 1 - odd)

    read_all(near)

    w_copy.wait()

    width = o_ref.shape[1] // chunks
    half = width // 2

    def place(axis, k):
        if axis == 0:
            return (y_me * nx + lax.rem(x_me + k, nx), c)
        return (lax.rem(y_me + k, ny) * nx + x_me, c)

    def offset(axis, k, other):
        return (other * nx + k) if axis == 0 else (k * nx + other)

    def first_move(j, h, k, other):
        at = (k - 1) * (ny if h == 0 else nx) + other
        out_buf, in_buf, send, recv = stage1[h]
        return pltpu.make_async_remote_copy(
            src_ref=out_buf.at[j, at], dst_ref=in_buf.at[j, at],
            send_sem=send.at[j, at], recv_sem=recv.at[j, at],
            device_id=place(h, k), device_id_type=MESH,
        )

    def second_move(j, h, k):
        out_buf, in_buf, send, recv = stage2[h]
        return pltpu.make_async_remote_copy(
            src_ref=out_buf.at[j, k - 1], dst_ref=in_buf.at[j, k - 1],
            send_sem=send.at[j, k - 1], recv_sem=recv.at[j, k - 1],
            device_id=place(1 - h, k), device_id_type=MESH,
        )

    sizes = ((nx, ny), (ny, nx))

    def projected(j, h, k, other):
        r = offset(h, k, other) * tokens
        at = pl.multiple_of(j * width + h * half, half)
        return jnp.dot(mixed[r : r + tokens, :], wv[:, pl.ds(at, half)], preferred_element_type=jnp.float32)

    def send_rows(others):
        def project(j, carry):
            for h, (n1, n2) in enumerate(sizes):
                for k in range(1, n1):
                    for other in others(n2):
                        y = projected(j, h, k, other)
                        stage1[h][0][j, (k - 1) * n2 + other] = y.astype(jnp.bfloat16)
                        first_move(j, h, k, other).start()
            return carry

        lax.fori_loop(0, chunks, project, 0)

    def keep_rows(j, carry):
        for h, (n1, n2) in enumerate(sizes):
            for other in range(n2):
                mine[h][j, other] = projected(j, h, 0, other)
        return carry

    send_rows(lambda n2: [0])
    for k in far:
        q_move(back(k)).wait_recv()
        features(k)
    read_all(far)
    send_rows(lambda n2: range(1, n2))
    read_all([0])
    lax.fori_loop(0, chunks, keep_rows, 0)

    def relay(j, carry):
        for h, (n1, n2) in enumerate(sizes):
            for other in range(1, n2):
                y = mine[h][j, other]
                for k in range(1, n1):
                    first_move(j, h, k, other).wait_recv()
                    y = y + stage1[h][1][j, (k - 1) * n2 + other].astype(jnp.float32)
                stage2[h][0][j, other - 1] = y.astype(jnp.bfloat16)
        for h, (n1, n2) in enumerate(sizes):
            for k in range(1, n2):
                second_move(j, h, k).start()
        return carry

    lax.fori_loop(0, chunks, relay, 0)

    def collect(j, carry):
        for h, (n1, n2) in enumerate(sizes):
            at = pl.multiple_of(j * width + h * half, half)
            y = mine[h][j, 0]
            for k in range(1, n1):
                first_move(j, h, k, 0).wait_recv()
                y = y + stage1[h][1][j, (k - 1) * n2].astype(jnp.float32)
            for k in range(1, n2):
                second_move(j, h, k).wait_recv()
                y = y + stage2[h][1][j, k - 1].astype(jnp.float32)
            o_ref[:, pl.ds(at, half)] = y.astype(jnp.bfloat16)
        return carry

    lax.fori_loop(0, chunks, collect, 0)

    for k in range(1, nb):
        q_move(k).wait_send()

    for j in range(messages):
        for k in range(1, nz + 1):
            pa_move(j, k).wait_send()
        for k in range(1, nz):
            rs_move(j, k).wait_send()
            ag_move(j, k)[1].wait_send()
        here, remote, _ = ag_move(j, 0)
        pl.when(jnp.logical_not(here))(remote.wait_send)
    for k in range(nb):
        for u in range(blocks // 2):
            fw_move(k, u).wait_send()

    def pr_end(j, carry):
        for h, (n1, n2) in enumerate(sizes):
            for k in range(1, n1):
                for other in range(n2):
                    first_move(j, h, k, other).wait_send()
            for k in range(1, n2):
                second_move(j, h, k).wait_send()
        return carry

    lax.fori_loop(0, chunks, pr_end, 0)


def solution(mesh):
    nb, nc = mesh.shape["batch"], mesh.shape["ctx"]
    nx = next(n for n in range(math.isqrt(nb), 0, -1) if nb % n == 0)
    ny = nb // nx

    def shards(asked_for, offered, contents, out_weight):
        _, tokens, heads, size = asked_for.shape
        rows = heads * size
        depth, columns = out_weight.shape
        pairs = rows // LANES
        width = CHUNK if columns % CHUNK == 0 else columns
        chunks = columns // width

        def flat(x):
            return x.transpose(0, 2, 3, 1).reshape(rows, tokens)

        bf16, f32 = jnp.bfloat16, jnp.float32
        dma = pltpu.SemaphoreType.DMA
        sizes = ((nx, ny), (ny, nx))

        def stage(blocks, moves):
            buffer = pltpu.VMEM((chunks, blocks, tokens, width // 2), bf16)
            return [buffer, buffer, dma((chunks, moves)), dma((chunks, moves))]

        half_pairs, ppg = nc // 2, pairs // nb
        spread = nb % 2 == 0 and ppg % half_pairs == 0 and ppg >= half_pairs
        held = ppg // half_pairs if spread else 1
        messages = pairs // nc // held
        high = held * size + EXTRA
        hops = pltpu.VMEM((messages, nc // 2, high, LANES), bf16)
        scratch = [
            pltpu.VMEM((rows, tokens), bf16),
            pltpu.VMEM((rows, tokens), bf16),
            pltpu.VMEM((depth, columns), bf16),
            pltpu.VMEM((nb, rows // nb, tokens), bf16),
            pltpu.VMEM((nb, ppg, tokens, LANES), bf16),
            hops,
            hops,
            hops,
            hops,
            pltpu.VMEM((messages, high, LANES), bf16),
            pltpu.VMEM((pairs // held, high, LANES), bf16),
            pltpu.VMEM((nb * tokens, rows // nb), bf16),
            [pltpu.VMEM((chunks, n2, tokens, width // 2), f32) for _, n2 in sizes],
            [stage((n1 - 1) * n2, (n1 - 1) * n2) for n1, n2 in sizes],
            [stage(n2 - 1, n2 - 1) for _, n2 in sizes],
            dma((4,)),
            dma((nb,)),
            dma((nb,)),
            dma((messages, nc // 2)),
            dma((messages, nc // 2)),
            dma((messages, nc // 2)),
            dma((messages, nc // 2)),
            dma((messages * nc // 2,)),
            dma((pairs // held,)),
            dma((pairs // held,)),
            dma((pairs // held,)),
        ]
        buffers = [x for x in jax.tree.leaves(scratch, is_leaf=lambda x: hasattr(x, "shape")) if x.dtype in (bf16, f32)]
        used = sum(math.prod(x.shape) * jnp.dtype(x.dtype).itemsize for x in buffers)
        limit = used + 4 * tokens * columns + 3 * 2**20

        out = pl.pallas_call(
            functools.partial(kernel, ny, nx, nc, size, (messages, held, spread)),
            out_shape=jax.ShapeDtypeStruct((tokens, columns), bf16),
            in_specs=[pl.BlockSpec(memory_space=pl.ANY)] * 4,
            out_specs=pl.BlockSpec(memory_space=pltpu.VMEM),
            scratch_shapes=scratch,
            compiler_params=pltpu.CompilerParams(
                collective_id=0, has_side_effects=True, vmem_limit_bytes=max(limit, 52 * 2**20)
            ),
        )(flat(asked_for), flat(offered), flat(contents), out_weight)
        return out[None]

    in_specs = (
        P("batch", "ctx", None, None),
        P("batch", "ctx", None, None),
        P("batch", "ctx", None, None),
        P("batch", None),
    )
    return jax.shard_map(
        shards, mesh=mesh, in_specs=in_specs, out_specs=P("batch", "ctx", None), check_vma=False
    )
```

```python
import functools
import math

import jax
import jax.numpy as jnp
from jax import lax
from jax.experimental import pallas as pl
from jax.experimental.pallas import tpu as pltpu
from jax.sharding import PartitionSpec as P

MESH = pl.DeviceIdType.MESH
LANES = 128
EXTRA = 8
CHUNK = 512
PIECES = 4
EARLY = 0


def softplus(x):
    x = x.astype(jnp.float32)
    return (jnp.maximum(x, 0.0) + jnp.log(1.0 + jnp.exp(-jnp.abs(x)))).astype(jnp.bfloat16)


def kernel(
    ny, nx, nc, size, grid, q_ref, k_ref, v_ref, w_ref, o_ref,
    kt, vt, wv, qx, ft, part, part_in, both, rs, own, st, mixed, mine, stage1, stage2,
    local_sem, load_sem, q_send, q_recv, pa_send, pa_recv, rs_send, rs_recv,
    ag_send, ag_recv, fw_send, fw_recv,
):
    b, c = lax.axis_index("batch"), lax.axis_index("ctx")
    nb = ny * nx
    rows, tokens = k_ref.shape
    pairs = rows // LANES
    ppg = pairs // nb
    share = rows // nb
    messages, held, rounds, spread = grid
    blocks = ppg // held
    base = held * size
    count = tokens * nc
    chunks = mine[0].shape[0]
    nz, z_me, odd = nc // 2, c // 2, lax.rem(c, 2)
    partner = z_me * 2 + 1 - odd
    y_me, x_me = b // nx, lax.rem(b, nx)

    def ahead(k):
        return lax.rem(y_me + k // nx, ny) * nx + lax.rem(x_me + k % nx, nx)

    def back(k):
        return (ny - k // nx) % ny * nx + (nx - k % nx) % nx

    near = [k for k in range(1, nb) if k < nx or k % nx == 0]
    far = [k for k in range(1, nb) if k not in near]
    order = near + far + [0]

    def load(i):
        at = pl.ds(ahead(order[i]) * share, share)
        return [
            pltpu.make_async_copy(ref.at[at], buffer.at[at], load_sem.at[n, i])
            for n, (ref, buffer) in enumerate(((k_ref, kt), (v_ref, vt)))
        ]

    q_copy = pltpu.make_async_copy(q_ref.at[pl.ds(b * share, share)], qx.at[0], local_sem.at[2])
    w_copy = pltpu.make_async_copy(w_ref, wv, local_sem.at[3])
    for i in range(nb):
        for copy in load(i):
            copy.start()
    q_copy.start()
    w_copy.start()

    barrier = pltpu.get_barrier_semaphore()

    def greet(device):
        pl.semaphore_signal(barrier, inc=1, device_id=device, device_id_type=MESH)

    greet((b, partner))
    for k in range(1, nb):
        greet((lax.rem(b + k, nb), c))
    for k in range(1, nz):
        greet((b, lax.rem(c + 2 * k, nc)))

    piece = share // PIECES

    def q_move(k, n):
        to = ahead(k)
        at = pl.ds(pl.multiple_of(to * share + n * piece, piece), piece)
        return pltpu.make_async_remote_copy(
            src_ref=q_ref.at[at], dst_ref=qx.at[back(k), pl.ds(n * piece, piece)],
            send_sem=q_send.at[k, n], recv_sem=q_recv.at[back(k), n],
            device_id=(to, c), device_id_type=MESH,
        )

    lane = lax.broadcasted_iota(jnp.int32, (size, LANES), 1) < size
    row_x = lax.broadcasted_iota(jnp.int32, (EXTRA, LANES), 0)
    ones = jnp.ones((2 * EXTRA, tokens), jnp.bfloat16)

    def first_pair(j, owner):
        if spread:
            even, uneven = order[j // rounds * 2], order[j // rounds * 2 + 1]
            group = jnp.where(lax.rem(owner, 2) == 0, ahead(even), ahead(uneven))
            return group * ppg + (owner // 2 * rounds + j % rounds) * held
        return j * nc + owner

    urgent = min(rounds, messages) if spread else 1
    late = 1 if messages > urgent and rounds > 1 else 0

    def pa_move(j, k):
        return pltpu.make_async_remote_copy(
            src_ref=part.at[j, k - 1], dst_ref=part_in.at[j, k - 1],
            send_sem=pa_send.at[j, k - 1], recv_sem=pa_recv.at[j, k - 1],
            device_id=(b, partner), device_id_type=MESH,
        )

    def rs_move(j, k):
        return pltpu.make_async_remote_copy(
            src_ref=both.at[j, k - 1], dst_ref=rs.at[j, k - 1],
            send_sem=rs_send.at[j, k - 1], recv_sem=rs_recv.at[j, k - 1],
            device_id=(b, lax.rem(z_me + k, nz) * 2 + odd), device_id_type=MESH,
        )

    def partial_sum(p):
        at = pl.multiple_of(p * LANES, LANES)
        feature = softplus(kt[pl.ds(at, LANES), :])
        left = jnp.concatenate([vt[pl.ds(at, LANES), :], ones], axis=0)
        s = lax.dot_general(left, feature, (((1,), (1,)), ((), ())), preferred_element_type=jnp.float32)
        return jnp.where(lane, s[:size], s[size : 2 * size]), s[2 * size : 2 * size + EXTRA]

    def split_mass(masses):
        packed = jnp.zeros((EXTRA, LANES), jnp.float32)
        for t, m in enumerate(masses):
            high = m.astype(jnp.bfloat16).astype(jnp.float32)
            packed = jnp.where(row_x == 2 * t, high, jnp.where(row_x == 2 * t + 1, m - high, packed))
        return packed.astype(jnp.bfloat16)

    def states_of(block):
        return [block[t * size : (t + 1) * size].astype(jnp.float32) for t in range(held)]

    def masses_of(block):
        extra = block[base:].astype(jnp.float32)
        return [extra[2 * t : 2 * t + 1] + extra[2 * t + 1 : 2 * t + 2] for t in range(held)]

    batches = [range(j, min(j + rounds, messages)) for j in range(0, messages, rounds)]

    def sum_for_partner(batch):
        def for_partner(k, carry):
            owner = lax.rem(z_me + k, nz) * 2 + 1 - odd
            for j in batch:
                sums = [partial_sum(first_pair(j, owner) + t) for t in range(held)]
                for t, (state, _) in enumerate(sums):
                    part[j, k - 1, t * size : (t + 1) * size, :] = state.astype(jnp.bfloat16)
                part[j, k - 1, base:, :] = split_mass([m for _, m in sums])
            return carry

        lax.fori_loop(1, nz + 1, for_partner, 0, unroll=1)

    def sum_for_chips(batch):
        def for_chip(k, carry):
            owner = lax.rem(z_me + k, nz) * 2 + odd
            sums = {j: [partial_sum(first_pair(j, owner) + t) for t in range(held)] for j in batch}
            for j in batch:
                pa_move(j, k).wait_recv()
            for j in batch:
                block = part_in[j, k - 1]
                for t, ((state, _), other) in enumerate(zip(sums[j], states_of(block))):
                    both[j, k - 1, t * size : (t + 1) * size, :] = (state + other).astype(jnp.bfloat16)
                both[j, k - 1, base:, :] = split_mass([m + o for (_, m), o in zip(sums[j], masses_of(block))])

            @pl.when(k < nz)
            def _():
                rs_move(batch[0], k).start()

            return carry

        lax.fori_loop(1, nz + 1, for_chip, 0, unroll=1)
        for j in batch[1:]:
            if j < messages - late:
                for k in range(1, nz):
                    rs_move(j, k).start()

    def start_partner(batch):
        for j in batch:
            for k in range(1, nz + 1):
                pa_move(j, k).start()

    per = -(-nb // len(batches)) if spread else nb
    for n, batch in enumerate(batches):
        for i in range(n * per, min(n * per + per, nb)):
            for copy in load(i):
                copy.wait()
        sum_for_partner(batch)
        if n == 0:
            pl.semaphore_wait(barrier, nb + nz - 1)
        start_partner(batch)
        if n == 0:
            for k in near:
                for m in range(PIECES):
                    q_move(k, m).start()
        sum_for_chips(batch)

    def features(k):
        span = ppg // PIECES
        for n in range(PIECES):
            if k > 0:
                q_move(back(k), n).wait_recv()

            def featured(i, carry):
                at = pl.multiple_of(i * LANES, LANES)
                ft[k, i] = softplus(qx[k, pl.ds(at, LANES), :]).T
                return carry

            lax.fori_loop(n * span, (n + 1) * span, featured, 0, unroll=True)

    q_copy.wait()
    features(0)

    def ag_move(j, k):
        p = first_pair(j, c)
        g = p // ppg
        block = lax.rem(p, ppg) // held
        side = lax.rem(block, 2)
        to = lax.rem(z_me + k, nz) * 2 + side
        landing = b * blocks + block
        remote = pltpu.make_async_remote_copy(
            src_ref=own.at[j], dst_ref=st.at[landing],
            send_sem=ag_send.at[j * nz + k], recv_sem=ag_recv.at[landing],
            device_id=(g, to), device_id_type=MESH,
        )
        local = pltpu.make_async_copy(own.at[j], st.at[landing], ag_recv.at[landing])
        here = jnp.logical_and(g == b, side == odd)
        return here, remote, local

    for j in range(messages):
        for k in range(1, nz):
            rs_move(j, k).wait_recv()
        parts = [both[j, nz - 1]] + [rs[j, k - 1] for k in range(1, nz)]
        states = [sum(x) / count for x in zip(*[states_of(p) for p in parts])]
        masses = [sum(x) / count for x in zip(*[masses_of(p) for p in parts])]
        for t, state in enumerate(states):
            own[j, t * size : (t + 1) * size, :] = state.astype(jnp.bfloat16)
        own[j, base:, :] = split_mass([jnp.broadcast_to(m, (EXTRA, LANES)) for m in masses])
        for k in range(1, nz):
            ag_move(j, k)[1].start()
        here, remote, local = ag_move(j, 0)
        pl.when(jnp.logical_not(here))(remote.start)
        pl.when(here)(local.start)
        if j == urgent - 1:
            for i in range(messages - late, messages):
                for k in range(1, nz):
                    rs_move(i, k).start()
            for k in far:
                for n in range(EARLY, PIECES):
                    q_move(k, n).start()
            for k in near:
                features(k)

    def fw_move(k, u):
        landing = ahead(k) * blocks + 2 * u + odd
        return pltpu.make_async_remote_copy(
            src_ref=st.at[landing], dst_ref=st.at[landing],
            send_sem=fw_send.at[landing], recv_sem=fw_recv.at[landing],
            device_id=(b, partner), device_id_type=MESH,
        )

    def read(found):
        products = []
        for k, block in found:
            at = ahead(k) * blocks + block
            for t in range(held):
                state = st[at, t * size : (t + 1) * size, :]
                mass = st[at, base:, :].astype(jnp.float32)
                mass = jnp.broadcast_to(mass[2 * t : 2 * t + 1], (size, LANES)).astype(jnp.bfloat16)
                zero = jnp.zeros_like(state)
                right = jnp.concatenate(
                    [jnp.where(lane, x, zero) if low else jnp.where(lane, zero, x)
                     for x in (state, mass) for low in (True, False)], axis=0,
                )
                slot = block * held + t
                y = lax.dot_general(
                    ft[k, slot], right, (((1,), (1,)), ((), ())), preferred_element_type=jnp.float32
                )
                products.append((k, slot, y))
        for k, slot, y in products:
            y = y[:, :LANES] * (count**0.5 / (y[:, LANES:] + 0.001))
            column = pl.multiple_of(slot * LANES, LANES)
            mixed[k * tokens : (k + 1) * tokens, pl.ds(column, LANES)] = y.astype(jnp.bfloat16)

    def read_all(sequences):
        found = [(k, u) for u in range(blocks // 2) for k in sequences]
        step = max(1, 4 // held)
        for n in range(0, len(found), step):
            for k, u in found[n : n + step]:
                at = ahead(k) * blocks + 2 * u + odd
                pltpu.make_async_copy(st.at[at], st.at[at], ag_recv.at[at]).wait()
                fw_move(k, u).start()
            read([(k, 2 * u + odd) for k, u in found[n : n + step]])
        step = max(1, 8 // held)
        for n in range(0, len(found), step):
            for k, u in found[n : n + step]:
                at = ahead(k) * blocks + 2 * u + 1 - odd
                pltpu.make_async_copy(st.at[at], st.at[at], fw_recv.at[at]).wait()
            read([(k, 2 * u + 1 - odd) for k, u in found[n : n + step]])

    read_all(near)

    w_copy.wait()

    width = o_ref.shape[1] // chunks
    half = width // 2

    def place(axis, k):
        if axis == 0:
            return (y_me * nx + lax.rem(x_me + k, nx), c)
        return (lax.rem(y_me + k, ny) * nx + x_me, c)

    def offset(axis, k, other):
        return (other * nx + k) if axis == 0 else (k * nx + other)

    def first_move(j, h, k, other):
        at = (k - 1) * (ny if h == 0 else nx) + other
        out_buf, in_buf, send, recv = stage1[h]
        return pltpu.make_async_remote_copy(
            src_ref=out_buf.at[j, at], dst_ref=in_buf.at[j, at],
            send_sem=send.at[j, at], recv_sem=recv.at[j, at],
            device_id=place(h, k), device_id_type=MESH,
        )

    def second_move(j, h, k):
        out_buf, in_buf, send, recv = stage2[h]
        return pltpu.make_async_remote_copy(
            src_ref=out_buf.at[j, k - 1], dst_ref=in_buf.at[j, k - 1],
            send_sem=send.at[j, k - 1], recv_sem=recv.at[j, k - 1],
            device_id=place(1 - h, k), device_id_type=MESH,
        )

    sizes = ((nx, ny), (ny, nx))

    def projected(j, h, k, other):
        r = offset(h, k, other) * tokens
        at = pl.multiple_of(j * width + h * half, half)
        return jnp.dot(mixed[r : r + tokens, :], wv[:, pl.ds(at, half)], preferred_element_type=jnp.float32)

    def send_rows(others):
        def project(j, carry):
            for h, (n1, n2) in enumerate(sizes):
                for k in range(1, n1):
                    for other in others(n2):
                        y = projected(j, h, k, other)
                        stage1[h][0][j, (k - 1) * n2 + other] = y.astype(jnp.bfloat16)
                        first_move(j, h, k, other).start()
            return carry

        lax.fori_loop(0, chunks, project, 0)

    def keep_rows(j, carry):
        for h, (n1, n2) in enumerate(sizes):
            for other in range(n2):
                mine[h][j, other] = projected(j, h, 0, other)
        return carry

    send_rows(lambda n2: [0])
    for k in far:
        features(k)
    read_all(far)
    send_rows(lambda n2: range(1, n2))
    read_all([0])
    lax.fori_loop(0, chunks, keep_rows, 0)

    def relay(j, carry):
        for h, (n1, n2) in enumerate(sizes):
            for other in range(1, n2):
                y = mine[h][j, other]
                for k in range(1, n1):
                    first_move(j, h, k, other).wait_recv()
                    y = y + stage1[h][1][j, (k - 1) * n2 + other].astype(jnp.float32)
                stage2[h][0][j, other - 1] = y.astype(jnp.bfloat16)
        for h, (n1, n2) in enumerate(sizes):
            for k in range(1, n2):
                second_move(j, h, k).start()
        return carry

    lax.fori_loop(0, chunks, relay, 0)

    def collect(j, carry):
        for h, (n1, n2) in enumerate(sizes):
            at = pl.multiple_of(j * width + h * half, half)
            y = mine[h][j, 0]
            for k in range(1, n1):
                first_move(j, h, k, 0).wait_recv()
                y = y + stage1[h][1][j, (k - 1) * n2].astype(jnp.float32)
            for k in range(1, n2):
                second_move(j, h, k).wait_recv()
                y = y + stage2[h][1][j, k - 1].astype(jnp.float32)
            o_ref[:, pl.ds(at, half)] = y.astype(jnp.bfloat16)
        return carry

    lax.fori_loop(0, chunks, collect, 0)

    for k in range(1, nb):
        for n in range(PIECES):
            q_move(k, n).wait_send()

    for j in range(messages):
        for k in range(1, nz + 1):
            pa_move(j, k).wait_send()
        for k in range(1, nz):
            rs_move(j, k).wait_send()
            ag_move(j, k)[1].wait_send()
        here, remote, _ = ag_move(j, 0)
        pl.when(jnp.logical_not(here))(remote.wait_send)
    for k in range(nb):
        for u in range(blocks // 2):
            fw_move(k, u).wait_send()

    def pr_end(j, carry):
        for h, (n1, n2) in enumerate(sizes):
            for k in range(1, n1):
                for other in range(n2):
                    first_move(j, h, k, other).wait_send()
            for k in range(1, n2):
                second_move(j, h, k).wait_send()
        return carry

    lax.fori_loop(0, chunks, pr_end, 0)


def solution(mesh):
    nb, nc = mesh.shape["batch"], mesh.shape["ctx"]
    nx = next(n for n in range(math.isqrt(nb), 0, -1) if nb % n == 0)
    ny = nb // nx

    def shards(asked_for, offered, contents, out_weight):
        _, tokens, heads, size = asked_for.shape
        rows = heads * size
        depth, columns = out_weight.shape
        pairs = rows // LANES
        width = CHUNK if columns % CHUNK == 0 else columns
        chunks = columns // width

        def flat(x):
            return x.transpose(0, 2, 3, 1).reshape(rows, tokens)

        bf16, f32 = jnp.bfloat16, jnp.float32
        dma = pltpu.SemaphoreType.DMA
        sizes = ((nx, ny), (ny, nx))

        def stage(blocks, moves):
            buffer = pltpu.VMEM((chunks, blocks, tokens, width // 2), bf16)
            return [buffer, buffer, dma((chunks, moves)), dma((chunks, moves))]

        half_pairs, ppg = nc // 2, pairs // nb
        spread = nb % 2 == 0 and ppg % half_pairs == 0 and ppg >= half_pairs
        held = ppg // half_pairs if spread else 1
        rounds = 1
        messages = pairs // nc // held
        high = held * size + EXTRA
        hops = pltpu.VMEM((messages, nc // 2, high, LANES), bf16)
        scratch = [
            pltpu.VMEM((rows, tokens), bf16),
            pltpu.VMEM((rows, tokens), bf16),
            pltpu.VMEM((depth, columns), bf16),
            pltpu.VMEM((nb, rows // nb, tokens), bf16),
            pltpu.VMEM((nb, ppg, tokens, LANES), bf16),
            hops,
            hops,
            hops,
            hops,
            pltpu.VMEM((messages, high, LANES), bf16),
            pltpu.VMEM((pairs // held, high, LANES), bf16),
            pltpu.VMEM((nb * tokens, rows // nb), bf16),
            [pltpu.VMEM((chunks, n2, tokens, width // 2), f32) for _, n2 in sizes],
            [stage((n1 - 1) * n2, (n1 - 1) * n2) for n1, n2 in sizes],
            [stage(n2 - 1, n2 - 1) for _, n2 in sizes],
            dma((4,)),
            dma((2, nb)),
            dma((nb, PIECES)),
            dma((nb, PIECES)),
            dma((messages, nc // 2)),
            dma((messages, nc // 2)),
            dma((messages, nc // 2)),
            dma((messages, nc // 2)),
            dma((messages * nc // 2,)),
            dma((pairs // held,)),
            dma((pairs // held,)),
            dma((pairs // held,)),
        ]
        buffers = [x for x in jax.tree.leaves(scratch, is_leaf=lambda x: hasattr(x, "shape")) if x.dtype in (bf16, f32)]
        used = sum(math.prod(x.shape) * jnp.dtype(x.dtype).itemsize for x in buffers)
        limit = used + 4 * tokens * columns + 3 * 2**20

        out = pl.pallas_call(
            functools.partial(kernel, ny, nx, nc, size, (messages, held, rounds, spread)),
            out_shape=jax.ShapeDtypeStruct((tokens, columns), bf16),
            in_specs=[pl.BlockSpec(memory_space=pl.ANY)] * 4,
            out_specs=pl.BlockSpec(memory_space=pltpu.VMEM),
            scratch_shapes=scratch,
            compiler_params=pltpu.CompilerParams(
                collective_id=0, has_side_effects=True, vmem_limit_bytes=max(limit, 52 * 2**20)
            ),
        )(flat(asked_for), flat(offered), flat(contents), out_weight)
        return out[None]

    in_specs = (
        P("batch", "ctx", None, None),
        P("batch", "ctx", None, None),
        P("batch", "ctx", None, None),
        P("batch", None),
    )
    return jax.shard_map(
        shards, mesh=mesh, in_specs=in_specs, out_specs=P("batch", "ctx", None), check_vma=False
    )
```

```python
import functools
import math

import jax
import jax.numpy as jnp
from jax import lax
from jax.experimental import pallas as pl
from jax.experimental.pallas import tpu as pltpu
from jax.sharding import PartitionSpec as P

MESH = pl.DeviceIdType.MESH
LANES = 128
EXTRA = 8
CHUNK = 1024
PIECES = 4


def softplus(x):
    x = x.astype(jnp.float32)
    return (jnp.maximum(x, 0.0) + jnp.log(1.0 + jnp.exp(-jnp.abs(x)))).astype(jnp.bfloat16)


def kernel(
    ny, nx, nc, size, grid, q_ref, k_ref, v_ref, w_ref, o_ref,
    kt, vt, wv, qx, ft, part, part_in, both, rs, own, st, mixed, mine, stage1, stage2,
    local_sem, load_sem, q_send, q_recv, pa_send, pa_recv, rs_send, rs_recv,
    ag_send, ag_recv, fw_send, fw_recv, relay_send,
):
    b, c = lax.axis_index("batch"), lax.axis_index("ctx")
    nb = ny * nx
    rows, tokens = k_ref.shape
    pairs = rows // LANES
    ppg = pairs // nb
    share = rows // nb
    messages, held, rounds, spread = grid
    blocks = ppg // held
    base = held * size
    count = tokens * nc
    chunks = mine[0].shape[0]
    nz, z_me, odd = nc // 2, c // 2, lax.rem(c, 2)
    partner = z_me * 2 + 1 - odd
    y_me, x_me = b // nx, lax.rem(b, nx)

    def ahead(k):
        return lax.rem(y_me + k // nx, ny) * nx + lax.rem(x_me + k % nx, nx)

    def back(k):
        return (ny - k // nx) % ny * nx + (nx - k % nx) % nx

    near = [k for k in range(1, nb) if k < nx or k % nx == 0]
    far = [k for k in range(1, nb) if k not in near]
    order = near + far + [0]

    def load(i):
        at = pl.ds(ahead(order[i]) * share, share)
        return [
            pltpu.make_async_copy(ref.at[at], buffer.at[at], load_sem.at[n, i])
            for n, (ref, buffer) in enumerate(((k_ref, kt), (v_ref, vt)))
        ]

    q_copy = pltpu.make_async_copy(q_ref.at[pl.ds(b * share, share)], qx.at[0], local_sem.at[2])
    w_copy = pltpu.make_async_copy(w_ref, wv, local_sem.at[3])
    for i in range(nb):
        for copy in load(i):
            copy.start()
    q_copy.start()
    w_copy.start()

    barrier = pltpu.get_barrier_semaphore()

    def greet(device):
        pl.semaphore_signal(barrier, inc=1, device_id=device, device_id_type=MESH)

    greet((b, partner))
    for k in range(1, nb):
        greet((lax.rem(b + k, nb), c))
    for k in range(1, nz):
        greet((b, lax.rem(c + 2 * k, nc)))

    pieces = math.gcd(PIECES, ppg)
    piece = share // pieces

    def q_move(k, n):
        to = ahead(k)
        at = pl.ds(pl.multiple_of(to * share + n * piece, piece), piece)
        return pltpu.make_async_remote_copy(
            src_ref=q_ref.at[at], dst_ref=qx.at[back(k), pl.ds(n * piece, piece)],
            send_sem=q_send.at[k, n], recv_sem=q_recv.at[back(k), n],
            device_id=(to, c), device_id_type=MESH,
        )

    lane = lax.broadcasted_iota(jnp.int32, (size, LANES), 1) < size
    row_x = lax.broadcasted_iota(jnp.int32, (EXTRA, LANES), 0)
    ones = jnp.ones((2 * EXTRA, tokens), jnp.bfloat16)

    def first_pair(j, owner):
        if spread:
            even, uneven = order[j // rounds * 2], order[j // rounds * 2 + 1]
            group = jnp.where(lax.rem(owner, 2) == 0, ahead(even), ahead(uneven))
            return group * ppg + (owner // 2 * rounds + j % rounds) * held
        return j * nc + owner

    urgent = rounds if spread and len(near) <= 2 * rounds else messages
    late = order[2 * urgent :] if urgent < messages else []

    def hop(i):
        down, up = nz - 1 - i, i
        down = jnp.where(down <= z_me, down - 1, down)
        up = jnp.where(up >= z_me, up + 1, up)
        k = lax.rem(jnp.where(2 * z_me < nz, down, up) - z_me + nz, nz)
        return jnp.where(i == nz - 1, nz, k)

    def pa_move(j, k):
        return pltpu.make_async_remote_copy(
            src_ref=part.at[j, k - 1], dst_ref=part_in.at[j, k - 1],
            send_sem=pa_send.at[j, k - 1], recv_sem=pa_recv.at[j, k - 1],
            device_id=(b, partner), device_id_type=MESH,
        )

    def rs_move(j, k):
        return pltpu.make_async_remote_copy(
            src_ref=both.at[j, k - 1], dst_ref=rs.at[j, k - 1],
            send_sem=rs_send.at[j, k - 1], recv_sem=rs_recv.at[j, k - 1],
            device_id=(b, lax.rem(z_me + k, nz) * 2 + odd), device_id_type=MESH,
        )

    def partial_sum(p):
        at = pl.multiple_of(p * LANES, LANES)
        feature = softplus(kt[pl.ds(at, LANES), :])
        left = jnp.concatenate([vt[pl.ds(at, LANES), :], ones], axis=0)
        s = lax.dot_general(left, feature, (((1,), (1,)), ((), ())), preferred_element_type=jnp.float32)
        return jnp.where(lane, s[:size], s[size : 2 * size]), s[2 * size : 2 * size + EXTRA]

    def split_mass(masses):
        packed = jnp.zeros((EXTRA, LANES), jnp.float32)
        for t, m in enumerate(masses):
            high = m.astype(jnp.bfloat16).astype(jnp.float32)
            packed = jnp.where(row_x == 2 * t, high, jnp.where(row_x == 2 * t + 1, m - high, packed))
        return packed.astype(jnp.bfloat16)

    def states_of(block):
        return [block[t * size : (t + 1) * size].astype(jnp.float32) for t in range(held)]

    def masses_of(block):
        extra = block[base:].astype(jnp.float32)
        return [extra[2 * t : 2 * t + 1] + extra[2 * t + 1 : 2 * t + 2] for t in range(held)]

    batches = [range(j, min(j + rounds, messages)) for j in range(0, messages, rounds)]

    def sum_for_partner(batch):
        def for_partner(i, carry):
            k = hop(i)
            owner = lax.rem(z_me + k, nz) * 2 + 1 - odd
            for j in batch:
                sums = [partial_sum(first_pair(j, owner) + t) for t in range(held)]
                for t, (state, _) in enumerate(sums):
                    part[j, k - 1, t * size : (t + 1) * size, :] = state.astype(jnp.bfloat16)
                part[j, k - 1, base:, :] = split_mass([m for _, m in sums])
            return carry

        lax.fori_loop(0, nz, for_partner, 0)

    def sum_for_chips(batch):
        def for_chip(i, carry):
            k = hop(i)
            owner = lax.rem(z_me + k, nz) * 2 + odd
            sums = {j: [partial_sum(first_pair(j, owner) + t) for t in range(held)] for j in batch}
            for j in batch:
                pa_move(j, k).wait_recv()
            for j in batch:
                block = part_in[j, k - 1]
                for t, ((state, _), other) in enumerate(zip(sums[j], states_of(block))):
                    both[j, k - 1, t * size : (t + 1) * size, :] = (state + other).astype(jnp.bfloat16)
                both[j, k - 1, base:, :] = split_mass([m + o for (_, m), o in zip(sums[j], masses_of(block))])

            @pl.when(i < nz - 1)
            def _():
                rs_move(batch[0], k).start()

            return carry

        lax.fori_loop(0, nz, for_chip, 0)
        for j in batch[1:]:
            if True:
                for k in range(1, nz):
                    rs_move(j, k).start()

    def start_partner(batch):
        for j in batch:
            for i in range(nz):
                pa_move(j, hop(i)).start()

    per = -(-nb // len(batches)) if spread else nb
    for n, batch in enumerate(batches):
        for i in range(n * per, min(n * per + per, nb)):
            for copy in load(i):
                copy.wait()
        sum_for_partner(batch)
        if n == 0:
            pl.semaphore_wait(barrier, nb + nz - 1)
        start_partner(batch)
        if n == 0:
            for k in near:
                for m in range(pieces):
                    q_move(k, m).start()
        sum_for_chips(batch)

    def features(k):
        span = ppg // pieces
        for n in range(pieces):
            if k > 0:
                q_move(back(k), n).wait_recv()

            def featured(i, carry):
                at = pl.multiple_of(i * LANES, LANES)
                ft[k, i] = softplus(qx[k, pl.ds(at, LANES), :]).T
                return carry

            lax.fori_loop(n * span, (n + 1) * span, featured, 0, unroll=True)

    q_copy.wait()
    features(0)

    def ag_move(j, k):
        p = first_pair(j, c)
        g = p // ppg
        block = lax.rem(p, ppg) // held
        side = lax.rem(block, 2)
        to = lax.rem(z_me + k, nz) * 2 + side
        landing = b * blocks + block
        remote = pltpu.make_async_remote_copy(
            src_ref=own.at[j], dst_ref=st.at[landing],
            send_sem=ag_send.at[j * nz + k], recv_sem=ag_recv.at[landing],
            device_id=(g, to), device_id_type=MESH,
        )
        local = pltpu.make_async_copy(own.at[j], st.at[landing], ag_recv.at[landing])
        here = jnp.logical_and(g == b, side == odd)
        return here, remote, local

    for j in range(messages):
        for k in range(1, nz):
            rs_move(j, k).wait_recv()
        parts = [both[j, nz - 1]] + [rs[j, k - 1] for k in range(1, nz)]
        states = [sum(x) / count for x in zip(*[states_of(p) for p in parts])]
        masses = [sum(x) / count for x in zip(*[masses_of(p) for p in parts])]
        for t, state in enumerate(states):
            own[j, t * size : (t + 1) * size, :] = state.astype(jnp.bfloat16)
        own[j, base:, :] = split_mass([jnp.broadcast_to(m, (EXTRA, LANES)) for m in masses])
        for i in range(nz - 1 if j < urgent else 0):
            ag_move(j, hop(i))[1].start()
        here, remote, local = ag_move(j, 0)
        pl.when(jnp.logical_not(here))(remote.start)
        pl.when(here)(local.start)
        if j == urgent - 1:
            for k in far:
                for n in range(pieces):
                    q_move(k, n).start()
            for k in near:
                features(k)

    relays = lax.rem(z_me, 2) == odd

    def relay_move(k, i):
        landing = ahead(k) * blocks + z_me
        return pltpu.make_async_remote_copy(
            src_ref=st.at[landing], dst_ref=st.at[landing],
            send_sem=relay_send.at[k, i], recv_sem=ag_recv.at[landing],
            device_id=(b, lax.rem(z_me + hop(i), nz) * 2 + odd), device_id_type=MESH,
        )

    def relay_states():
        for k in late:
            at = ahead(k) * blocks + z_me
            pltpu.make_async_copy(st.at[at], st.at[at], ag_recv.at[at]).wait()
            for i in range(nz - 1):
                relay_move(k, i).start()

    def fw_move(k, u):
        landing = ahead(k) * blocks + 2 * u + odd
        return pltpu.make_async_remote_copy(
            src_ref=st.at[landing], dst_ref=st.at[landing],
            send_sem=fw_send.at[landing], recv_sem=fw_recv.at[landing],
            device_id=(b, partner), device_id_type=MESH,
        )

    def read(found):
        products = []
        for k, block in found:
            at = ahead(k) * blocks + block
            for t in range(held):
                state = st[at, t * size : (t + 1) * size, :]
                mass = st[at, base:, :].astype(jnp.float32)
                mass = jnp.broadcast_to(mass[2 * t : 2 * t + 1], (size, LANES)).astype(jnp.bfloat16)
                zero = jnp.zeros_like(state)
                right = jnp.concatenate(
                    [jnp.where(lane, x, zero) if low else jnp.where(lane, zero, x)
                     for x in (state, mass) for low in (True, False)], axis=0,
                )
                slot = block * held + t
                y = lax.dot_general(
                    ft[k, slot], right, (((1,), (1,)), ((), ())), preferred_element_type=jnp.float32
                )
                products.append((k, slot, y))
        for k, slot, y in products:
            y = y[:, :LANES] * (count**0.5 / (y[:, LANES:] + 0.001))
            column = pl.multiple_of(slot * LANES, LANES)
            mixed[k * tokens : (k + 1) * tokens, pl.ds(column, LANES)] = y.astype(jnp.bfloat16)

    def read_all(sequences):
        found = [(k, u) for u in range(blocks // 2) for k in sequences]
        step = max(1, 4 // held)
        for n in range(0, len(found), step):
            for k, u in found[n : n + step]:
                at = ahead(k) * blocks + 2 * u + odd
                arrival = pltpu.make_async_copy(st.at[at], st.at[at], ag_recv.at[at])
                if k in late:
                    pl.when(2 * u + odd != z_me)(arrival.wait)
                else:
                    arrival.wait()
                fw_move(k, u).start()
            read([(k, 2 * u + odd) for k, u in found[n : n + step]])
        step = max(1, 8 // held)
        for n in range(0, len(found), step):
            for k, u in found[n : n + step]:
                at = ahead(k) * blocks + 2 * u + 1 - odd
                pltpu.make_async_copy(st.at[at], st.at[at], fw_recv.at[at]).wait()
            read([(k, 2 * u + 1 - odd) for k, u in found[n : n + step]])

    read_all(near)

    w_copy.wait()

    width = o_ref.shape[1] // chunks
    half = width // 2

    def place(axis, k):
        if axis == 0:
            return (y_me * nx + lax.rem(x_me + k, nx), c)
        return (lax.rem(y_me + k, ny) * nx + x_me, c)

    def offset(axis, k, other):
        return (other * nx + k) if axis == 0 else (k * nx + other)

    def first_move(j, h, k, other):
        at = (k - 1) * (ny if h == 0 else nx) + other
        out_buf, in_buf, send, recv = stage1[h]
        return pltpu.make_async_remote_copy(
            src_ref=out_buf.at[j, at], dst_ref=in_buf.at[j, at],
            send_sem=send.at[j, at], recv_sem=recv.at[j, at],
            device_id=place(h, k), device_id_type=MESH,
        )

    def second_move(j, h, k):
        out_buf, in_buf, send, recv = stage2[h]
        return pltpu.make_async_remote_copy(
            src_ref=out_buf.at[j, k - 1], dst_ref=in_buf.at[j, k - 1],
            send_sem=send.at[j, k - 1], recv_sem=recv.at[j, k - 1],
            device_id=place(1 - h, k), device_id_type=MESH,
        )

    sizes = ((nx, ny), (ny, nx))

    def projected(j, h, k, other):
        r = offset(h, k, other) * tokens
        at = pl.multiple_of(j * width + h * half, half)
        return jnp.dot(mixed[r : r + tokens, :], wv[:, pl.ds(at, half)], preferred_element_type=jnp.float32)

    def send_rows(others):
        def project(j, carry):
            for h, (n1, n2) in enumerate(sizes):
                for k in range(1, n1):
                    for other in others(n2):
                        y = projected(j, h, k, other)
                        stage1[h][0][j, (k - 1) * n2 + other] = y.astype(jnp.bfloat16)
                        first_move(j, h, k, other).start()
            return carry

        lax.fori_loop(0, chunks, project, 0)

    def keep_rows(j, carry):
        for h, (n1, n2) in enumerate(sizes):
            for other in range(n2):
                mine[h][j, other] = projected(j, h, 0, other)
        return carry

    send_rows(lambda n2: [0])
    pl.when(relays)(relay_states)
    for k in far:
        features(k)
    read_all(far)
    send_rows(lambda n2: range(1, n2))
    read_all([0])
    lax.fori_loop(0, chunks, keep_rows, 0)

    def relay(j, carry):
        for h, (n1, n2) in enumerate(sizes):
            for other in range(1, n2):
                y = mine[h][j, other]
                for k in range(1, n1):
                    first_move(j, h, k, other).wait_recv()
                    y = y + stage1[h][1][j, (k - 1) * n2 + other].astype(jnp.float32)
                stage2[h][0][j, other - 1] = y.astype(jnp.bfloat16)
        for h, (n1, n2) in enumerate(sizes):
            for k in range(1, n2):
                second_move(j, h, k).start()
        return carry

    lax.fori_loop(0, chunks, relay, 0)

    def collect(j, carry):
        for h, (n1, n2) in enumerate(sizes):
            at = pl.multiple_of(j * width + h * half, half)
            y = mine[h][j, 0]
            for k in range(1, n1):
                first_move(j, h, k, 0).wait_recv()
                y = y + stage1[h][1][j, (k - 1) * n2].astype(jnp.float32)
            for k in range(1, n2):
                second_move(j, h, k).wait_recv()
                y = y + stage2[h][1][j, k - 1].astype(jnp.float32)
            o_ref[:, pl.ds(at, half)] = y.astype(jnp.bfloat16)
        return carry

    lax.fori_loop(0, chunks, collect, 0)

    for k in range(1, nb):
        for n in range(pieces):
            q_move(k, n).wait_send()

    for j in range(messages):
        for k in range(1, nz + 1):
            pa_move(j, k).wait_send()
        for k in range(1, nz):
            rs_move(j, k).wait_send()
            if j < urgent:
                ag_move(j, k)[1].wait_send()
        here, remote, _ = ag_move(j, 0)
        pl.when(jnp.logical_not(here))(remote.wait_send)
    for k in range(nb):
        for u in range(blocks // 2):
            fw_move(k, u).wait_send()

    @pl.when(relays)
    def _():
        for k in late:
            for i in range(nz - 1):
                relay_move(k, i).wait_send()

    def pr_end(j, carry):
        for h, (n1, n2) in enumerate(sizes):
            for k in range(1, n1):
                for other in range(n2):
                    first_move(j, h, k, other).wait_send()
            for k in range(1, n2):
                second_move(j, h, k).wait_send()
        return carry

    lax.fori_loop(0, chunks, pr_end, 0)


def solution(mesh):
    nb, nc = mesh.shape["batch"], mesh.shape["ctx"]
    nx = next(n for n in range(math.isqrt(nb), 0, -1) if nb % n == 0)
    ny = nb // nx

    def shards(asked_for, offered, contents, out_weight):
        _, tokens, heads, size = asked_for.shape
        rows = heads * size
        depth, columns = out_weight.shape
        pairs = rows // LANES
        width = CHUNK if columns % CHUNK == 0 else columns
        chunks = columns // width

        def flat(x):
            return x.transpose(0, 2, 3, 1).reshape(rows, tokens)

        bf16, f32 = jnp.bfloat16, jnp.float32
        dma = pltpu.SemaphoreType.DMA
        sizes = ((nx, ny), (ny, nx))

        def stage(blocks, moves):
            buffer = pltpu.VMEM((chunks, blocks, tokens, width // 2), bf16)
            return [buffer, buffer, dma((chunks, moves)), dma((chunks, moves))]

        half_pairs, ppg = nc // 2, pairs // nb
        spread = nb % 2 == 0 and ppg % half_pairs == 0 and ppg >= half_pairs
        held = ppg // half_pairs if spread else 1
        rounds = 1
        messages = pairs // nc // held
        high = held * size + EXTRA
        hops = pltpu.VMEM((messages, nc // 2, high, LANES), bf16)
        scratch = [
            pltpu.VMEM((rows, tokens), bf16),
            pltpu.VMEM((rows, tokens), bf16),
            pltpu.VMEM((depth, columns), bf16),
            pltpu.VMEM((nb, rows // nb, tokens), bf16),
            pltpu.VMEM((nb, ppg, tokens, LANES), bf16),
            hops,
            hops,
            hops,
            hops,
            pltpu.VMEM((messages, high, LANES), bf16),
            pltpu.VMEM((pairs // held, high, LANES), bf16),
            pltpu.VMEM((nb * tokens, rows // nb), bf16),
            [pltpu.VMEM((chunks, n2, tokens, width // 2), f32) for _, n2 in sizes],
            [stage((n1 - 1) * n2, (n1 - 1) * n2) for n1, n2 in sizes],
            [stage(n2 - 1, n2 - 1) for _, n2 in sizes],
            dma((4,)),
            dma((2, nb)),
            dma((nb, math.gcd(PIECES, ppg))),
            dma((nb, math.gcd(PIECES, ppg))),
            dma((messages, nc // 2)),
            dma((messages, nc // 2)),
            dma((messages, nc // 2)),
            dma((messages, nc // 2)),
            dma((messages * nc // 2,)),
            dma((pairs // held,)),
            dma((pairs // held,)),
            dma((pairs // held,)),
            dma((nb, nc // 2)),
        ]
        buffers = [x for x in jax.tree.leaves(scratch, is_leaf=lambda x: hasattr(x, "shape")) if x.dtype in (bf16, f32)]
        used = sum(math.prod(x.shape) * jnp.dtype(x.dtype).itemsize for x in buffers)
        limit = used + 4 * tokens * columns + 3 * 2**20

        out = pl.pallas_call(
            functools.partial(kernel, ny, nx, nc, size, (messages, held, rounds, spread)),
            out_shape=jax.ShapeDtypeStruct((tokens, columns), bf16),
            in_specs=[pl.BlockSpec(memory_space=pl.ANY)] * 4,
            out_specs=pl.BlockSpec(memory_space=pltpu.VMEM),
            scratch_shapes=scratch,
            compiler_params=pltpu.CompilerParams(
                collective_id=0, has_side_effects=True, vmem_limit_bytes=max(limit, 52 * 2**20)
            ),
        )(flat(asked_for), flat(offered), flat(contents), out_weight)
        return out[None]

    in_specs = (
        P("batch", "ctx", None, None),
        P("batch", "ctx", None, None),
        P("batch", "ctx", None, None),
        P("batch", None),
    )
    return jax.shard_map(
        shards, mesh=mesh, in_specs=in_specs, out_specs=P("batch", "ctx", None), check_vma=False
    )
```

```python
import functools
import math

import jax
import jax.numpy as jnp
from jax import lax
from jax.experimental import pallas as pl
from jax.experimental.pallas import tpu as pltpu
from jax.sharding import PartitionSpec as P

MESH = pl.DeviceIdType.MESH
LANES = 128
EXTRA = 8
CHUNK = 1024
PIECES = 1


def softplus(x):
    x = x.astype(jnp.float32)
    return (jnp.maximum(x, 0.0) + jnp.log(1.0 + jnp.exp(-jnp.abs(x)))).astype(jnp.bfloat16)


def kernel(
    ny, nx, nc, size, grid, q_ref, k_ref, v_ref, w_ref, o_ref,
    kt, vt, wv, qx, ft, part, part_in, both, rs, own, st, mixed, mine, stage1, stage2,
    local_sem, load_sem, q_send, q_recv, pa_send, pa_recv, rs_send, rs_recv,
    ag_send, ag_recv, fw_send, fw_recv, relay_send,
):
    b, c = lax.axis_index("batch"), lax.axis_index("ctx")
    nb = ny * nx
    rows, tokens = k_ref.shape
    pairs = rows // LANES
    ppg = pairs // nb
    share = rows // nb
    messages, held, rounds, spread = grid
    blocks = ppg // held
    base = held * size
    count = tokens * nc
    chunks = mine[0].shape[0]
    nz, z_me, odd = nc // 2, c // 2, lax.rem(c, 2)
    partner = z_me * 2 + 1 - odd
    y_me, x_me = b // nx, lax.rem(b, nx)

    def ahead(k):
        return lax.rem(y_me + k // nx, ny) * nx + lax.rem(x_me + k % nx, nx)

    def back(k):
        return (ny - k // nx) % ny * nx + (nx - k % nx) % nx

    near = [k for k in range(1, nb) if k < nx or k % nx == 0]
    far = [k for k in range(1, nb) if k not in near]
    order = near + far + [0]

    def load(i):
        at = pl.ds(ahead(order[i]) * share, share)
        return [
            pltpu.make_async_copy(ref.at[at], buffer.at[at], load_sem.at[n, i])
            for n, (ref, buffer) in enumerate(((k_ref, kt), (v_ref, vt)))
        ]

    q_copy = pltpu.make_async_copy(q_ref.at[pl.ds(b * share, share)], qx.at[0], local_sem.at[2])
    w_copy = pltpu.make_async_copy(w_ref, wv, local_sem.at[3])
    batches = [range(j, min(j + rounds, messages)) for j in range(0, messages, rounds)]
    per = -(-nb // len(batches)) if spread else nb
    for i in range(per):
        for copy in load(i):
            copy.start()

    barrier = pltpu.get_barrier_semaphore()

    def greet(device):
        pl.semaphore_signal(barrier, inc=1, device_id=device, device_id_type=MESH)

    greet((b, partner))
    for k in range(1, nb):
        greet((lax.rem(b + k, nb), c))
    for k in range(1, nz):
        greet((b, lax.rem(c + 2 * k, nc)))

    pieces = math.gcd(PIECES, ppg)
    piece = share // pieces

    def q_move(k, n):
        to = ahead(k)
        at = pl.ds(pl.multiple_of(to * share + n * piece, piece), piece)
        return pltpu.make_async_remote_copy(
            src_ref=q_ref.at[at], dst_ref=qx.at[back(k), pl.ds(n * piece, piece)],
            send_sem=q_send.at[k, n], recv_sem=q_recv.at[back(k), n],
            device_id=(to, c), device_id_type=MESH,
        )

    lane = lax.broadcasted_iota(jnp.int32, (size, LANES), 1) < size
    row_x = lax.broadcasted_iota(jnp.int32, (EXTRA, LANES), 0)
    ones = jnp.ones((2 * EXTRA, tokens), jnp.bfloat16)

    def first_pair(j, owner):
        if spread:
            even, uneven = order[j // rounds * 2], order[j // rounds * 2 + 1]
            group = jnp.where(lax.rem(owner, 2) == 0, ahead(even), ahead(uneven))
            return group * ppg + (owner // 2 * rounds + j % rounds) * held
        return j * nc + owner

    urgent = rounds if spread and len(near) <= 2 * rounds else messages
    late = order[2 * urgent :] if urgent < messages else []

    def hop(i):
        down, up = nz - 1 - i, i
        down = jnp.where(down <= z_me, down - 1, down)
        up = jnp.where(up >= z_me, up + 1, up)
        k = lax.rem(jnp.where(2 * z_me < nz, down, up) - z_me + nz, nz)
        return jnp.where(i == nz - 1, nz, k)

    def pa_move(j, k):
        return pltpu.make_async_remote_copy(
            src_ref=part.at[j, k - 1], dst_ref=part_in.at[j, k - 1],
            send_sem=pa_send.at[j, k - 1], recv_sem=pa_recv.at[j, k - 1],
            device_id=(b, partner), device_id_type=MESH,
        )

    def rs_move(j, k):
        return pltpu.make_async_remote_copy(
            src_ref=both.at[j, k - 1], dst_ref=rs.at[j, k - 1],
            send_sem=rs_send.at[j, k - 1], recv_sem=rs_recv.at[j, k - 1],
            device_id=(b, lax.rem(z_me + k, nz) * 2 + odd), device_id_type=MESH,
        )

    def partial_sum(p):
        at = pl.multiple_of(p * LANES, LANES)
        feature = softplus(kt[pl.ds(at, LANES), :])
        left = jnp.concatenate([vt[pl.ds(at, LANES), :], ones], axis=0)
        s = lax.dot_general(left, feature, (((1,), (1,)), ((), ())), preferred_element_type=jnp.float32)
        return jnp.where(lane, s[:size], s[size : 2 * size]), s[2 * size : 2 * size + EXTRA]

    def split_mass(masses):
        packed = jnp.zeros((EXTRA, LANES), jnp.float32)
        for t, m in enumerate(masses):
            high = m.astype(jnp.bfloat16).astype(jnp.float32)
            packed = jnp.where(row_x == 2 * t, high, jnp.where(row_x == 2 * t + 1, m - high, packed))
        return packed.astype(jnp.bfloat16)

    def states_of(block):
        return [block[t * size : (t + 1) * size].astype(jnp.float32) for t in range(held)]

    def masses_of(block):
        extra = block[base:].astype(jnp.float32)
        return [extra[2 * t : 2 * t + 1] + extra[2 * t + 1 : 2 * t + 2] for t in range(held)]


    def sum_for_partner(batch):
        def for_partner(i, carry):
            k = hop(i)
            owner = lax.rem(z_me + k, nz) * 2 + 1 - odd
            for j in batch:
                sums = [partial_sum(first_pair(j, owner) + t) for t in range(held)]
                for t, (state, _) in enumerate(sums):
                    part[j, k - 1, t * size : (t + 1) * size, :] = state.astype(jnp.bfloat16)
                part[j, k - 1, base:, :] = split_mass([m for _, m in sums])
            return carry

        lax.fori_loop(0, nz, for_partner, 0)

    def sum_for_chips(batch):
        def for_chip(i, carry):
            k = hop(i)
            owner = lax.rem(z_me + k, nz) * 2 + odd
            sums = {j: [partial_sum(first_pair(j, owner) + t) for t in range(held)] for j in batch}
            for j in batch:
                pa_move(j, k).wait_recv()
            for j in batch:
                block = part_in[j, k - 1]
                for t, ((state, _), other) in enumerate(zip(sums[j], states_of(block))):
                    both[j, k - 1, t * size : (t + 1) * size, :] = (state + other).astype(jnp.bfloat16)
                both[j, k - 1, base:, :] = split_mass([m + o for (_, m), o in zip(sums[j], masses_of(block))])

            @pl.when(i < nz - 1)
            def _():
                rs_move(batch[0], k).start()

            return carry

        lax.fori_loop(0, nz, for_chip, 0)
        for j in batch[1:]:
            if True:
                for k in range(1, nz):
                    rs_move(j, k).start()

    def start_partner(batch):
        for j in batch:
            for i in range(nz):
                pa_move(j, hop(i)).start()

    for n, batch in enumerate(batches):
        for i in range(n * per, min(n * per + per, nb)):
            for copy in load(i):
                copy.wait()
        if n == 0:
            for i in range(per, nb):
                for copy in load(i):
                    copy.start()
            q_copy.start()
        sum_for_partner(batch)
        if n == 0:
            pl.semaphore_wait(barrier, nb + nz - 1)
        start_partner(batch)
        if n == 0:
            for k in near:
                for m in range(pieces):
                    q_move(k, m).start()
        sum_for_chips(batch)
        if n == 0:
            w_copy.start()

    def features(k):
        span = ppg // pieces
        for n in range(pieces):
            if k > 0:
                q_move(back(k), n).wait_recv()

            def featured(i, carry):
                at = pl.multiple_of(i * LANES, LANES)
                ft[k, i] = softplus(qx[k, pl.ds(at, LANES), :]).T
                return carry

            lax.fori_loop(n * span, (n + 1) * span, featured, 0, unroll=True)

    q_copy.wait()
    features(0)

    def ag_move(j, k):
        p = first_pair(j, c)
        g = p // ppg
        block = lax.rem(p, ppg) // held
        side = lax.rem(block, 2)
        to = lax.rem(z_me + k, nz) * 2 + side
        landing = b * blocks + block
        remote = pltpu.make_async_remote_copy(
            src_ref=own.at[j], dst_ref=st.at[landing],
            send_sem=ag_send.at[j * nz + k], recv_sem=ag_recv.at[landing],
            device_id=(g, to), device_id_type=MESH,
        )
        local = pltpu.make_async_copy(own.at[j], st.at[landing], ag_recv.at[landing])
        here = jnp.logical_and(g == b, side == odd)
        return here, remote, local

    for j in range(messages):
        for k in range(1, nz):
            rs_move(j, k).wait_recv()
        parts = [both[j, nz - 1]] + [rs[j, k - 1] for k in range(1, nz)]
        states = [sum(x) / count for x in zip(*[states_of(p) for p in parts])]
        masses = [sum(x) / count for x in zip(*[masses_of(p) for p in parts])]
        for t, state in enumerate(states):
            own[j, t * size : (t + 1) * size, :] = state.astype(jnp.bfloat16)
        own[j, base:, :] = split_mass([jnp.broadcast_to(m, (EXTRA, LANES)) for m in masses])
        for i in range(nz - 1 if j < urgent else 0):
            ag_move(j, hop(i))[1].start()
        here, remote, local = ag_move(j, 0)
        pl.when(jnp.logical_not(here))(remote.start)
        pl.when(here)(local.start)
        if j == urgent - 1:
            for k in near:
                features(k)
            for k in far:
                for n in range(pieces):
                    q_move(k, n).start()

    relays = lax.rem(z_me, 2) == odd

    def relay_move(k, i):
        landing = ahead(k) * blocks + z_me
        return pltpu.make_async_remote_copy(
            src_ref=st.at[landing], dst_ref=st.at[landing],
            send_sem=relay_send.at[k, i], recv_sem=ag_recv.at[landing],
            device_id=(b, lax.rem(z_me + hop(i), nz) * 2 + odd), device_id_type=MESH,
        )

    def relay_states():
        for k in late:
            at = ahead(k) * blocks + z_me
            pltpu.make_async_copy(st.at[at], st.at[at], ag_recv.at[at]).wait()
            for i in range(nz - 1):
                relay_move(k, i).start()

    def fw_move(k, u):
        landing = ahead(k) * blocks + 2 * u + odd
        return pltpu.make_async_remote_copy(
            src_ref=st.at[landing], dst_ref=st.at[landing],
            send_sem=fw_send.at[landing], recv_sem=fw_recv.at[landing],
            device_id=(b, partner), device_id_type=MESH,
        )

    def read(found):
        products = []
        for k, block in found:
            at = ahead(k) * blocks + block
            for t in range(held):
                state = st[at, t * size : (t + 1) * size, :]
                mass = st[at, base:, :].astype(jnp.float32)
                mass = jnp.broadcast_to(mass[2 * t : 2 * t + 1], (size, LANES)).astype(jnp.bfloat16)
                zero = jnp.zeros_like(state)
                right = jnp.concatenate(
                    [jnp.where(lane, x, zero) if low else jnp.where(lane, zero, x)
                     for x in (state, mass) for low in (True, False)], axis=0,
                )
                slot = block * held + t
                y = lax.dot_general(
                    ft[k, slot], right, (((1,), (1,)), ((), ())), preferred_element_type=jnp.float32
                )
                products.append((k, slot, y))
        for k, slot, y in products:
            y = y[:, :LANES] * (count**0.5 / (y[:, LANES:] + 0.001))
            column = pl.multiple_of(slot * LANES, LANES)
            mixed[k * tokens : (k + 1) * tokens, pl.ds(column, LANES)] = y.astype(jnp.bfloat16)

    def read_all(sequences):
        found = [(k, u) for u in range(blocks // 2) for k in sequences]
        step = max(1, 4 // held)
        for n in range(0, len(found), step):
            for k, u in found[n : n + step]:
                at = ahead(k) * blocks + 2 * u + odd
                arrival = pltpu.make_async_copy(st.at[at], st.at[at], ag_recv.at[at])
                if k in late:
                    pl.when(2 * u + odd != z_me)(arrival.wait)
                else:
                    arrival.wait()
                fw_move(k, u).start()
            read([(k, 2 * u + odd) for k, u in found[n : n + step]])
        step = max(1, 8 // held)
        for n in range(0, len(found), step):
            for k, u in found[n : n + step]:
                at = ahead(k) * blocks + 2 * u + 1 - odd
                pltpu.make_async_copy(st.at[at], st.at[at], fw_recv.at[at]).wait()
            read([(k, 2 * u + 1 - odd) for k, u in found[n : n + step]])

    read_all(near)

    w_copy.wait()

    width = o_ref.shape[1] // chunks
    half = width // 2

    def place(axis, k):
        if axis == 0:
            return (y_me * nx + lax.rem(x_me + k, nx), c)
        return (lax.rem(y_me + k, ny) * nx + x_me, c)

    def offset(axis, k, other):
        return (other * nx + k) if axis == 0 else (k * nx + other)

    def first_move(j, h, k, other):
        at = (k - 1) * (ny if h == 0 else nx) + other
        out_buf, in_buf, send, recv = stage1[h]
        return pltpu.make_async_remote_copy(
            src_ref=out_buf.at[j, at], dst_ref=in_buf.at[j, at],
            send_sem=send.at[j, at], recv_sem=recv.at[j, at],
            device_id=place(h, k), device_id_type=MESH,
        )

    def second_move(j, h, k):
        out_buf, in_buf, send, recv = stage2[h]
        return pltpu.make_async_remote_copy(
            src_ref=out_buf.at[j, k - 1], dst_ref=in_buf.at[j, k - 1],
            send_sem=send.at[j, k - 1], recv_sem=recv.at[j, k - 1],
            device_id=place(1 - h, k), device_id_type=MESH,
        )

    sizes = ((nx, ny), (ny, nx))

    def projected(j, h, k, other):
        r = offset(h, k, other) * tokens
        at = pl.multiple_of(j * width + h * half, half)
        return jnp.dot(mixed[r : r + tokens, :], wv[:, pl.ds(at, half)], preferred_element_type=jnp.float32)

    def send_rows(others):
        def project(j, carry):
            for h, (n1, n2) in enumerate(sizes):
                for k in range(1, n1):
                    for other in others(n2):
                        y = projected(j, h, k, other)
                        stage1[h][0][j, (k - 1) * n2 + other] = y.astype(jnp.bfloat16)
                        first_move(j, h, k, other).start()
            return carry

        lax.fori_loop(0, chunks, project, 0)

    def keep_rows(j, carry):
        for h, (n1, n2) in enumerate(sizes):
            for other in range(n2):
                mine[h][j, other] = projected(j, h, 0, other)
        return carry

    send_rows(lambda n2: [0])
    pl.when(relays)(relay_states)
    for k in far:
        features(k)
    read_all(far)
    send_rows(lambda n2: range(1, n2))
    read_all([0])
    lax.fori_loop(0, chunks, keep_rows, 0)

    def relay(j, carry):
        for h, (n1, n2) in enumerate(sizes):
            for other in range(1, n2):
                y = mine[h][j, other]
                for k in range(1, n1):
                    first_move(j, h, k, other).wait_recv()
                    y = y + stage1[h][1][j, (k - 1) * n2 + other].astype(jnp.float32)
                stage2[h][0][j, other - 1] = y.astype(jnp.bfloat16)
        for h, (n1, n2) in enumerate(sizes):
            for k in range(1, n2):
                second_move(j, h, k).start()
        return carry

    lax.fori_loop(0, chunks, relay, 0)

    def collect(j, carry):
        for h, (n1, n2) in enumerate(sizes):
            at = pl.multiple_of(j * width + h * half, half)
            y = mine[h][j, 0]
            for k in range(1, n1):
                first_move(j, h, k, 0).wait_recv()
                y = y + stage1[h][1][j, (k - 1) * n2].astype(jnp.float32)
            for k in range(1, n2):
                second_move(j, h, k).wait_recv()
                y = y + stage2[h][1][j, k - 1].astype(jnp.float32)
            o_ref[:, pl.ds(at, half)] = y.astype(jnp.bfloat16)
        return carry

    lax.fori_loop(0, chunks, collect, 0)

    for k in range(1, nb):
        for n in range(pieces):
            q_move(k, n).wait_send()

    for j in range(messages):
        for k in range(1, nz + 1):
            pa_move(j, k).wait_send()
        for k in range(1, nz):
            rs_move(j, k).wait_send()
            if j < urgent:
                ag_move(j, k)[1].wait_send()
        here, remote, _ = ag_move(j, 0)
        pl.when(jnp.logical_not(here))(remote.wait_send)
    for k in range(nb):
        for u in range(blocks // 2):
            fw_move(k, u).wait_send()

    @pl.when(relays)
    def _():
        for k in late:
            for i in range(nz - 1):
                relay_move(k, i).wait_send()

    def pr_end(j, carry):
        for h, (n1, n2) in enumerate(sizes):
            for k in range(1, n1):
                for other in range(n2):
                    first_move(j, h, k, other).wait_send()
            for k in range(1, n2):
                second_move(j, h, k).wait_send()
        return carry

    lax.fori_loop(0, chunks, pr_end, 0)


def solution(mesh):
    nb, nc = mesh.shape["batch"], mesh.shape["ctx"]
    nx = next(n for n in range(math.isqrt(nb), 0, -1) if nb % n == 0)
    ny = nb // nx

    def shards(asked_for, offered, contents, out_weight):
        _, tokens, heads, size = asked_for.shape
        rows = heads * size
        depth, columns = out_weight.shape
        pairs = rows // LANES
        width = CHUNK if columns % CHUNK == 0 else columns
        chunks = columns // width

        def flat(x):
            return x.transpose(0, 2, 3, 1).reshape(rows, tokens)

        bf16, f32 = jnp.bfloat16, jnp.float32
        dma = pltpu.SemaphoreType.DMA
        sizes = ((nx, ny), (ny, nx))

        def stage(blocks, moves):
            buffer = pltpu.VMEM((chunks, blocks, tokens, width // 2), bf16)
            return [buffer, buffer, dma((chunks, moves)), dma((chunks, moves))]

        half_pairs, ppg = nc // 2, pairs // nb
        spread = nb % 2 == 0 and ppg % half_pairs == 0 and ppg >= half_pairs
        held = ppg // half_pairs if spread else 1
        rounds = 1
        messages = pairs // nc // held
        high = held * size + EXTRA
        hops = pltpu.VMEM((messages, nc // 2, high, LANES), bf16)
        scratch = [
            pltpu.VMEM((rows, tokens), bf16),
            pltpu.VMEM((rows, tokens), bf16),
            pltpu.VMEM((depth, columns), bf16),
            pltpu.VMEM((nb, rows // nb, tokens), bf16),
            pltpu.VMEM((nb, ppg, tokens, LANES), bf16),
            hops,
            hops,
            hops,
            hops,
            pltpu.VMEM((messages, high, LANES), bf16),
            pltpu.VMEM((pairs // held, high, LANES), bf16),
            pltpu.VMEM((nb * tokens, rows // nb), bf16),
            [pltpu.VMEM((chunks, n2, tokens, width // 2), f32) for _, n2 in sizes],
            [stage((n1 - 1) * n2, (n1 - 1) * n2) for n1, n2 in sizes],
            [stage(n2 - 1, n2 - 1) for _, n2 in sizes],
            dma((4,)),
            dma((2, nb)),
            dma((nb, math.gcd(PIECES, ppg))),
            dma((nb, math.gcd(PIECES, ppg))),
            dma((messages, nc // 2)),
            dma((messages, nc // 2)),
            dma((messages, nc // 2)),
            dma((messages, nc // 2)),
            dma((messages * nc // 2,)),
            dma((pairs // held,)),
            dma((pairs // held,)),
            dma((pairs // held,)),
            dma((nb, nc // 2)),
        ]
        buffers = [x for x in jax.tree.leaves(scratch, is_leaf=lambda x: hasattr(x, "shape")) if x.dtype in (bf16, f32)]
        used = sum(math.prod(x.shape) * jnp.dtype(x.dtype).itemsize for x in buffers)
        limit = used + 4 * tokens * columns + 3 * 2**20

        out = pl.pallas_call(
            functools.partial(kernel, ny, nx, nc, size, (messages, held, rounds, spread)),
            out_shape=jax.ShapeDtypeStruct((tokens, columns), bf16),
            in_specs=[pl.BlockSpec(memory_space=pl.ANY)] * 4,
            out_specs=pl.BlockSpec(memory_space=pltpu.VMEM),
            scratch_shapes=scratch,
            compiler_params=pltpu.CompilerParams(
                collective_id=0, has_side_effects=True, vmem_limit_bytes=max(limit, 52 * 2**20)
            ),
        )(flat(asked_for), flat(offered), flat(contents), out_weight)
        return out[None]

    in_specs = (
        P("batch", "ctx", None, None),
        P("batch", "ctx", None, None),
        P("batch", "ctx", None, None),
        P("batch", None),
    )
    return jax.shard_map(
        shards, mesh=mesh, in_specs=in_specs, out_specs=P("batch", "ctx", None), check_vma=False
    )
```

```python
import functools
import math

import jax
import jax.numpy as jnp
from jax import lax
from jax.experimental import pallas as pl
from jax.experimental.pallas import tpu as pltpu
from jax.sharding import PartitionSpec as P

MESH = pl.DeviceIdType.MESH
LANES = 128
EXTRA = 8
CHUNK = 1024
PIECES = 1


def softplus(x):
    x = x.astype(jnp.float32)
    return (jnp.maximum(x, 0.0) + jnp.log(1.0 + jnp.exp(-jnp.abs(x)))).astype(jnp.bfloat16)


def kernel(
    ny, nx, nc, size, grid, q_ref, k_ref, v_ref, w_ref, o_ref,
    kt, vt, wv, qx, ft, part, part_in, both, rs, own, st, mixed, mine, stage1, stage2,
    local_sem, load_sem, q_send, q_recv, pa_send, pa_recv, rs_send, rs_recv,
    ag_send, ag_recv, fw_send, fw_recv, relay_send,
):
    b, c = lax.axis_index("batch"), lax.axis_index("ctx")
    nb = ny * nx
    rows, tokens = k_ref.shape
    pairs = rows // LANES
    ppg = pairs // nb
    share = rows // nb
    messages, held, rounds, spread = grid
    blocks = ppg // held
    base = held * size
    count = tokens * nc
    chunks = mine[0].shape[0]
    nz, z_me, odd = nc // 2, c // 2, lax.rem(c, 2)
    partner = z_me * 2 + 1 - odd
    y_me, x_me = b // nx, lax.rem(b, nx)

    def ahead(k):
        return lax.rem(y_me + k // nx, ny) * nx + lax.rem(x_me + k % nx, nx)

    def back(k):
        return (ny - k // nx) % ny * nx + (nx - k % nx) % nx

    near = [k for k in range(1, nb) if k < nx or k % nx == 0]
    far = [k for k in range(1, nb) if k not in near]
    order = near + far + [0]

    def load(i):
        at = pl.ds(ahead(order[i]) * share, share)
        return [
            pltpu.make_async_copy(ref.at[at], buffer.at[at], load_sem.at[n, i])
            for n, (ref, buffer) in enumerate(((k_ref, kt), (v_ref, vt)))
        ]

    q_copy = pltpu.make_async_copy(q_ref.at[pl.ds(b * share, share)], qx.at[0], local_sem.at[2])
    w_copy = pltpu.make_async_copy(w_ref, wv, local_sem.at[3])
    batches = [range(j, min(j + rounds, messages)) for j in range(0, messages, rounds)]
    per = -(-nb // len(batches)) if spread else nb
    for i in range(per):
        for copy in load(i):
            copy.start()

    barrier = pltpu.get_barrier_semaphore()

    def greet(device):
        pl.semaphore_signal(barrier, inc=1, device_id=device, device_id_type=MESH)

    greet((b, partner))
    for k in range(1, nb):
        greet((lax.rem(b + k, nb), c))
    for k in range(1, nz):
        greet((b, lax.rem(c + 2 * k, nc)))

    pieces = math.gcd(PIECES, ppg)
    piece = share // pieces

    def q_move(k, n):
        to = ahead(k)
        at = pl.ds(pl.multiple_of(to * share + n * piece, piece), piece)
        return pltpu.make_async_remote_copy(
            src_ref=q_ref.at[at], dst_ref=qx.at[back(k), pl.ds(n * piece, piece)],
            send_sem=q_send.at[k, n], recv_sem=q_recv.at[back(k), n],
            device_id=(to, c), device_id_type=MESH,
        )

    lane = lax.broadcasted_iota(jnp.int32, (size, LANES), 1) < size
    row_x = lax.broadcasted_iota(jnp.int32, (EXTRA, LANES), 0)
    ones = jnp.ones((2 * EXTRA, tokens), jnp.bfloat16)

    def first_pair(j, owner):
        if spread:
            even, uneven = order[j // rounds * 2], order[j // rounds * 2 + 1]
            group = jnp.where(lax.rem(owner, 2) == 0, ahead(even), ahead(uneven))
            return group * ppg + (owner // 2 * rounds + j % rounds) * held
        return j * nc + owner

    urgent = rounds if spread and len(near) <= 2 * rounds else messages
    late = order[2 * urgent :] if urgent < messages else []

    def hop(i):
        down, up = nz - 1 - i, i
        down = jnp.where(down <= z_me, down - 1, down)
        up = jnp.where(up >= z_me, up + 1, up)
        k = lax.rem(jnp.where(2 * z_me < nz, down, up) - z_me + nz, nz)
        return jnp.where(i == nz - 1, nz, k)

    def pa_move(j, k):
        return pltpu.make_async_remote_copy(
            src_ref=part.at[j, k - 1], dst_ref=part_in.at[j, k - 1],
            send_sem=pa_send.at[j, k - 1], recv_sem=pa_recv.at[j, k - 1],
            device_id=(b, partner), device_id_type=MESH,
        )

    def rs_move(j, k):
        return pltpu.make_async_remote_copy(
            src_ref=both.at[j, k - 1], dst_ref=rs.at[j, k - 1],
            send_sem=rs_send.at[j, k - 1], recv_sem=rs_recv.at[j, k - 1],
            device_id=(b, lax.rem(z_me + k, nz) * 2 + odd), device_id_type=MESH,
        )

    def partial_sum(p):
        at = pl.multiple_of(p * LANES, LANES)
        feature = softplus(kt[pl.ds(at, LANES), :])
        left = jnp.concatenate([vt[pl.ds(at, LANES), :], ones], axis=0)
        s = lax.dot_general(left, feature, (((1,), (1,)), ((), ())), preferred_element_type=jnp.float32)
        return jnp.where(lane, s[:size], s[size : 2 * size]), s[2 * size : 2 * size + EXTRA]

    def split_mass(masses):
        packed = jnp.zeros((EXTRA, LANES), jnp.float32)
        for t, m in enumerate(masses):
            high = m.astype(jnp.bfloat16).astype(jnp.float32)
            packed = jnp.where(row_x == 2 * t, high, jnp.where(row_x == 2 * t + 1, m - high, packed))
        return packed.astype(jnp.bfloat16)

    def states_of(block):
        return [block[t * size : (t + 1) * size].astype(jnp.float32) for t in range(held)]

    def masses_of(block):
        extra = block[base:].astype(jnp.float32)
        return [extra[2 * t : 2 * t + 1] + extra[2 * t + 1 : 2 * t + 2] for t in range(held)]


    def sum_for_partner(batch):
        def for_partner(i, carry):
            k = hop(i)
            owner = lax.rem(z_me + k, nz) * 2 + 1 - odd
            for j in batch:
                sums = [partial_sum(first_pair(j, owner) + t) for t in range(held)]
                for t, (state, _) in enumerate(sums):
                    part[j, k - 1, t * size : (t + 1) * size, :] = state.astype(jnp.bfloat16)
                part[j, k - 1, base:, :] = split_mass([m for _, m in sums])
            return carry

        lax.fori_loop(0, nz, for_partner, 0)

    def sum_for_chips(batch):
        def for_chip(i, carry):
            k = hop(i)
            owner = lax.rem(z_me + k, nz) * 2 + odd
            sums = {j: [partial_sum(first_pair(j, owner) + t) for t in range(held)] for j in batch}
            for j in batch:
                pa_move(j, k).wait_recv()
            for j in batch:
                block = part_in[j, k - 1]
                for t, ((state, _), other) in enumerate(zip(sums[j], states_of(block))):
                    both[j, k - 1, t * size : (t + 1) * size, :] = (state + other).astype(jnp.bfloat16)
                both[j, k - 1, base:, :] = split_mass([m + o for (_, m), o in zip(sums[j], masses_of(block))])

            @pl.when(i < nz - 1)
            def _():
                rs_move(batch[0], k).start()

            return carry

        lax.fori_loop(0, nz, for_chip, 0)
        for j in batch[1:]:
            if True:
                for k in range(1, nz):
                    rs_move(j, k).start()

    def start_partner(batch):
        for j in batch:
            for i in range(nz):
                pa_move(j, hop(i)).start()

    for n, batch in enumerate(batches):
        for i in range(n * per, min(n * per + per, nb)):
            for copy in load(i):
                copy.wait()
        if n == 0:
            for i in range(per, nb):
                for copy in load(i):
                    copy.start()
            q_copy.start()
        sum_for_partner(batch)
        if n == 0:
            pl.semaphore_wait(barrier, nb + nz - 1)
        start_partner(batch)
        if n == 0:
            for k in near:
                for m in range(pieces):
                    q_move(k, m).start()
        sum_for_chips(batch)
        if n == 0:
            w_copy.start()

    def features(k):
        span = ppg // pieces
        for n in range(pieces):
            if k > 0:
                q_move(back(k), n).wait_recv()

            def featured(i, carry):
                at = pl.multiple_of(i * LANES, LANES)
                ft[k, i] = softplus(qx[k, pl.ds(at, LANES), :]).T
                return carry

            lax.fori_loop(n * span, (n + 1) * span, featured, 0, unroll=True)

    q_copy.wait()
    features(0)

    def ag_move(j, k):
        p = first_pair(j, c)
        g = p // ppg
        block = lax.rem(p, ppg) // held
        side = lax.rem(block, 2)
        to = lax.rem(z_me + k, nz) * 2 + side
        landing = b * blocks + block
        remote = pltpu.make_async_remote_copy(
            src_ref=own.at[j], dst_ref=st.at[landing],
            send_sem=ag_send.at[j * nz + k], recv_sem=ag_recv.at[landing],
            device_id=(g, to), device_id_type=MESH,
        )
        local = pltpu.make_async_copy(own.at[j], st.at[landing], ag_recv.at[landing])
        here = jnp.logical_and(g == b, side == odd)
        return here, remote, local

    for j in range(messages):
        for k in range(1, nz):
            rs_move(j, k).wait_recv()
        parts = [both[j, nz - 1]] + [rs[j, k - 1] for k in range(1, nz)]
        states = [sum(x) / count for x in zip(*[states_of(p) for p in parts])]
        masses = [sum(x) / count for x in zip(*[masses_of(p) for p in parts])]
        for t, state in enumerate(states):
            own[j, t * size : (t + 1) * size, :] = state.astype(jnp.bfloat16)
        own[j, base:, :] = split_mass([jnp.broadcast_to(m, (EXTRA, LANES)) for m in masses])
        here, remote, local = ag_move(j, 0)
        pl.when(jnp.logical_not(here))(remote.start)
        pl.when(here)(local.start)
        for i in range(nz - 1 if j < urgent else 0):
            ag_move(j, hop(i))[1].start()
        if j == urgent - 1:
            for k in near:
                features(k)
            for k in far:
                for n in range(pieces):
                    q_move(k, n).start()

    relays = lax.rem(z_me, 2) == odd

    def relay_move(k, i):
        landing = ahead(k) * blocks + z_me
        return pltpu.make_async_remote_copy(
            src_ref=st.at[landing], dst_ref=st.at[landing],
            send_sem=relay_send.at[k, i], recv_sem=ag_recv.at[landing],
            device_id=(b, lax.rem(z_me + hop(i), nz) * 2 + odd), device_id_type=MESH,
        )

    def relay_states():
        for k in late:
            at = ahead(k) * blocks + z_me
            pltpu.make_async_copy(st.at[at], st.at[at], ag_recv.at[at]).wait()
            for i in range(nz - 1):
                relay_move(k, i).start()

    def fw_move(k, u):
        landing = ahead(k) * blocks + 2 * u + odd
        return pltpu.make_async_remote_copy(
            src_ref=st.at[landing], dst_ref=st.at[landing],
            send_sem=fw_send.at[landing], recv_sem=fw_recv.at[landing],
            device_id=(b, partner), device_id_type=MESH,
        )

    def read(found):
        products = []
        for k, block in found:
            at = ahead(k) * blocks + block
            for t in range(held):
                state = st[at, t * size : (t + 1) * size, :]
                mass = st[at, base:, :].astype(jnp.float32)
                mass = jnp.broadcast_to(mass[2 * t : 2 * t + 1], (size, LANES)).astype(jnp.bfloat16)
                zero = jnp.zeros_like(state)
                right = jnp.concatenate(
                    [jnp.where(lane, x, zero) if low else jnp.where(lane, zero, x)
                     for x in (state, mass) for low in (True, False)], axis=0,
                )
                slot = block * held + t
                y = lax.dot_general(
                    ft[k, slot], right, (((1,), (1,)), ((), ())), preferred_element_type=jnp.float32
                )
                products.append((k, slot, y))
        for k, slot, y in products:
            y = y[:, :LANES] * (count**0.5 / (y[:, LANES:] + 0.001))
            column = pl.multiple_of(slot * LANES, LANES)
            mixed[k * tokens : (k + 1) * tokens, pl.ds(column, LANES)] = y.astype(jnp.bfloat16)

    def read_all(sequences):
        found = [(k, u) for u in range(blocks // 2) for k in sequences]
        step = max(1, 4 // held)
        for n in range(0, len(found), step):
            for k, u in found[n : n + step]:
                at = ahead(k) * blocks + 2 * u + odd
                arrival = pltpu.make_async_copy(st.at[at], st.at[at], ag_recv.at[at])
                if k in late:
                    pl.when(2 * u + odd != z_me)(arrival.wait)
                else:
                    arrival.wait()
                fw_move(k, u).start()
            read([(k, 2 * u + odd) for k, u in found[n : n + step]])
        step = max(1, 8 // held)
        for n in range(0, len(found), step):
            for k, u in found[n : n + step]:
                at = ahead(k) * blocks + 2 * u + 1 - odd
                pltpu.make_async_copy(st.at[at], st.at[at], fw_recv.at[at]).wait()
            read([(k, 2 * u + 1 - odd) for k, u in found[n : n + step]])

    read_all(near)

    w_copy.wait()

    width = o_ref.shape[1] // chunks
    half = width // 2

    def place(axis, k):
        if axis == 0:
            return (y_me * nx + lax.rem(x_me + k, nx), c)
        return (lax.rem(y_me + k, ny) * nx + x_me, c)

    def offset(axis, k, other):
        return (other * nx + k) if axis == 0 else (k * nx + other)

    def first_move(j, h, k, other):
        at = (k - 1) * (ny if h == 0 else nx) + other
        out_buf, in_buf, send, recv = stage1[h]
        return pltpu.make_async_remote_copy(
            src_ref=out_buf.at[j, at], dst_ref=in_buf.at[j, at],
            send_sem=send.at[j, at], recv_sem=recv.at[j, at],
            device_id=place(h, k), device_id_type=MESH,
        )

    def second_move(j, h, k):
        out_buf, in_buf, send, recv = stage2[h]
        return pltpu.make_async_remote_copy(
            src_ref=out_buf.at[j, k - 1], dst_ref=in_buf.at[j, k - 1],
            send_sem=send.at[j, k - 1], recv_sem=recv.at[j, k - 1],
            device_id=place(1 - h, k), device_id_type=MESH,
        )

    sizes = ((nx, ny), (ny, nx))

    def projected(j, h, k, other):
        r = offset(h, k, other) * tokens
        at = pl.multiple_of(j * width + h * half, half)
        return jnp.dot(mixed[r : r + tokens, :], wv[:, pl.ds(at, half)], preferred_element_type=jnp.float32)

    def send_rows(others):
        def project(j, carry):
            for h, (n1, n2) in enumerate(sizes):
                for k in range(1, n1):
                    for other in others(n2):
                        y = projected(j, h, k, other)
                        stage1[h][0][j, (k - 1) * n2 + other] = y.astype(jnp.bfloat16)
                        first_move(j, h, k, other).start()
            return carry

        lax.fori_loop(0, chunks, project, 0)

    def keep_rows(j, carry):
        for h, (n1, n2) in enumerate(sizes):
            for other in range(n2):
                mine[h][j, other] = projected(j, h, 0, other)
        return carry

    send_rows(lambda n2: [0])
    pl.when(relays)(relay_states)
    for k in far:
        features(k)
    read_all(far)
    send_rows(lambda n2: range(1, n2))
    read_all([0])
    lax.fori_loop(0, chunks, keep_rows, 0)

    def relay(j, carry):
        for h, (n1, n2) in enumerate(sizes):
            for other in range(1, n2):
                y = mine[h][j, other]
                for k in range(1, n1):
                    first_move(j, h, k, other).wait_recv()
                    y = y + stage1[h][1][j, (k - 1) * n2 + other].astype(jnp.float32)
                stage2[h][0][j, other - 1] = y.astype(jnp.bfloat16)
        for h, (n1, n2) in enumerate(sizes):
            for k in range(1, n2):
                second_move(j, h, k).start()
        return carry

    lax.fori_loop(0, chunks, relay, 0)

    def collect(j, carry):
        for h, (n1, n2) in enumerate(sizes):
            at = pl.multiple_of(j * width + h * half, half)
            y = mine[h][j, 0]
            for k in range(1, n1):
                first_move(j, h, k, 0).wait_recv()
                y = y + stage1[h][1][j, (k - 1) * n2].astype(jnp.float32)
            for k in range(1, n2):
                second_move(j, h, k).wait_recv()
                y = y + stage2[h][1][j, k - 1].astype(jnp.float32)
            o_ref[:, pl.ds(at, half)] = y.astype(jnp.bfloat16)
        return carry

    lax.fori_loop(0, chunks, collect, 0)

    for k in range(1, nb):
        for n in range(pieces):
            q_move(k, n).wait_send()

    for j in range(messages):
        for k in range(1, nz + 1):
            pa_move(j, k).wait_send()
        for k in range(1, nz):
            rs_move(j, k).wait_send()
            if j < urgent:
                ag_move(j, k)[1].wait_send()
        here, remote, _ = ag_move(j, 0)
        pl.when(jnp.logical_not(here))(remote.wait_send)
    for k in range(nb):
        for u in range(blocks // 2):
            fw_move(k, u).wait_send()

    @pl.when(relays)
    def _():
        for k in late:
            for i in range(nz - 1):
                relay_move(k, i).wait_send()

    def pr_end(j, carry):
        for h, (n1, n2) in enumerate(sizes):
            for k in range(1, n1):
                for other in range(n2):
                    first_move(j, h, k, other).wait_send()
            for k in range(1, n2):
                second_move(j, h, k).wait_send()
        return carry

    lax.fori_loop(0, chunks, pr_end, 0)


def solution(mesh):
    nb, nc = mesh.shape["batch"], mesh.shape["ctx"]
    nx = next(n for n in range(math.isqrt(nb), 0, -1) if nb % n == 0)
    ny = nb // nx

    def shards(asked_for, offered, contents, out_weight):
        _, tokens, heads, size = asked_for.shape
        rows = heads * size
        depth, columns = out_weight.shape
        pairs = rows // LANES
        width = CHUNK if columns % CHUNK == 0 else columns
        chunks = columns // width

        def flat(x):
            return x.transpose(0, 2, 3, 1).reshape(rows, tokens)

        bf16, f32 = jnp.bfloat16, jnp.float32
        dma = pltpu.SemaphoreType.DMA
        sizes = ((nx, ny), (ny, nx))

        def stage(blocks, moves):
            buffer = pltpu.VMEM((chunks, blocks, tokens, width // 2), bf16)
            return [buffer, buffer, dma((chunks, moves)), dma((chunks, moves))]

        half_pairs, ppg = nc // 2, pairs // nb
        spread = nb % 2 == 0 and ppg % half_pairs == 0 and ppg >= half_pairs
        held = ppg // half_pairs if spread else 1
        rounds = 1
        messages = pairs // nc // held
        high = held * size + EXTRA
        hops = pltpu.VMEM((messages, nc // 2, high, LANES), bf16)
        scratch = [
            pltpu.VMEM((rows, tokens), bf16),
            pltpu.VMEM((rows, tokens), bf16),
            pltpu.VMEM((depth, columns), bf16),
            pltpu.VMEM((nb, rows // nb, tokens), bf16),
            pltpu.VMEM((nb, ppg, tokens, LANES), bf16),
            hops,
            hops,
            hops,
            hops,
            pltpu.VMEM((messages, high, LANES), bf16),
            pltpu.VMEM((pairs // held, high, LANES), bf16),
            pltpu.VMEM((nb * tokens, rows // nb), bf16),
            [pltpu.VMEM((chunks, n2, tokens, width // 2), f32) for _, n2 in sizes],
            [stage((n1 - 1) * n2, (n1 - 1) * n2) for n1, n2 in sizes],
            [stage(n2 - 1, n2 - 1) for _, n2 in sizes],
            dma((4,)),
            dma((2, nb)),
            dma((nb, math.gcd(PIECES, ppg))),
            dma((nb, math.gcd(PIECES, ppg))),
            dma((messages, nc // 2)),
            dma((messages, nc // 2)),
            dma((messages, nc // 2)),
            dma((messages, nc // 2)),
            dma((messages * nc // 2,)),
            dma((pairs // held,)),
            dma((pairs // held,)),
            dma((pairs // held,)),
            dma((nb, nc // 2)),
        ]
        buffers = [x for x in jax.tree.leaves(scratch, is_leaf=lambda x: hasattr(x, "shape")) if x.dtype in (bf16, f32)]
        used = sum(math.prod(x.shape) * jnp.dtype(x.dtype).itemsize for x in buffers)
        limit = used + 4 * tokens * columns + 3 * 2**20

        out = pl.pallas_call(
            functools.partial(kernel, ny, nx, nc, size, (messages, held, rounds, spread)),
            out_shape=jax.ShapeDtypeStruct((tokens, columns), bf16),
            in_specs=[pl.BlockSpec(memory_space=pl.ANY)] * 4,
            out_specs=pl.BlockSpec(memory_space=pltpu.VMEM),
            scratch_shapes=scratch,
            compiler_params=pltpu.CompilerParams(
                collective_id=0, has_side_effects=True, vmem_limit_bytes=max(limit, 52 * 2**20)
            ),
        )(flat(asked_for), flat(offered), flat(contents), out_weight)
        return out[None]

    in_specs = (
        P("batch", "ctx", None, None),
        P("batch", "ctx", None, None),
        P("batch", "ctx", None, None),
        P("batch", None),
    )
    return jax.shard_map(
        shards, mesh=mesh, in_specs=in_specs, out_specs=P("batch", "ctx", None), check_vma=False
    )
```
